128 devices in a mesh: res: 32 (over z, x, core), grp: 4 (over y).
Axes of the slice: x: 4, y: 4, z: 4, core: 2. Of those that a mesh axis runs over, the one named last changes fastest.
Arguments:
- right_side: float32 [3, 64, 64, 512], P(None, 'res', 'grp'), may hold values from -30 to 30
- accumulation: float32 [3, 3, 64, 64, 512], P(None, None, 'res', 'grp'), may hold values from -1 to 2, as said below
- transmissibility: float32 [6, 3, 3, 64, 64, 512], P(None, None, None, 'res', 'grp'), may hold values from -1 to 2, as said below
- completion: int32 [1024, 256], P(('res', 'grp')), may hold values from 0 to 16383, as said below
- live_count: int32 [1024], P(('res', 'grp')), may hold values from 64 to 256
- owner: int32 [1024, 1], P(('res', 'grp')), may hold values from 0 to 3; in each aligned block of 8 rows (0 to 7, 8 to 15, ...) at most 4 rows name the same one
- cell_to_well: float32 [1024, 3, 256], P(('res', 'grp')), may hold values from -3 to 3
- well_to_cell: float32 [1024, 3, 256], P(('res', 'grp')), may hold values from -3 to 3
- inverse: float32 [128, 4, 4, 256, 256], P(('res', 'grp')), may hold values from -1 to 2
Outputs:
- solution: float32 [3, 64, 64, 512], P(None, 'res', 'grp')
- residual: float32 [3, 64, 64, 512], P(None, 'res', 'grp')
The draws below stay inside these ranges and needn't reach their ends.
Inputs may be any that keep to these rules, and one draw needn't show every extreme that they name: `completion`: cells may repeat. Among the 8 wells of one device at most 4 name the same owner. `accumulation`: diagonal entries positive. `transmissibility`: diagonal entries positive.
All inputs are finite; a program needn't handle non-finite values.
Results may differ from the reference program's by a relative error of at most 0.0003.
Values sent between devices are 32-bit elements; how exact they have to be, the bound alone decides.
A program may use at most 128 MiB of HBM per device.

```python
import math
import jax
import jax.numpy as jnp
import numpy as np
from jax import lax

CX = 2
CY = 16
CZ = 512
COMP = 3
SEGB = 256
BH = 8
ITERS = 3
CAP = 4
NX = 64
NY = 64
NZ = 512
NBLK = 1024
N_RES = 32
N_GRP = 4
DEVICES = 128


def block_field(key, lead_shape):
    first, second = jax.random.split(key)
    cells = (NX, NY, NZ)
    diagonal = jnp.exp(jax.random.uniform(first, lead_shape + (COMP,) + cells, jnp.float32, math.log(0.5), math.log(2.0)))
    offdiag = 0.15 * jnp.clip(jax.random.normal(second, lead_shape + (COMP, COMP) + cells, jnp.float32), -4.0, 4.0)
    identity = jnp.eye(COMP, dtype=jnp.float32).reshape((1,) * len(lead_shape) + (COMP, COMP, 1, 1, 1))
    diagonal = jnp.expand_dims(diagonal, len(lead_shape) + 1)
    return identity * diagonal + (1.0 - identity) * offdiag


def draw_accumulation(key, part):
    return block_field(jax.random.fold_in(key, 11), ())


def draw_transmissibility(key, part):
    return block_field(jax.random.fold_in(key, 12), (6,))


def draw_right_side(key, part):
    first = jax.random.fold_in(jax.random.fold_in(key, 13), 0)
    grade = jnp.exp(math.log(3.0) * jnp.arange(NX, dtype=jnp.float32) / NX)[None, :, None, None]
    return jnp.clip(jax.random.normal(first, (COMP, NX, NY, NZ), jnp.float32), -6.0, 6.0) * grade


def draw_completion(key, part):
    first, second, third = jax.random.split(jax.random.fold_in(key, 14), 3)
    cell_x = jax.random.randint(first, (NBLK, SEGB), 0, CX, dtype=jnp.int32)
    cell_y = jax.random.randint(second, (NBLK, SEGB), 0, CY, dtype=jnp.int32)
    cell_z = jax.random.randint(third, (NBLK, SEGB), 0, CZ, dtype=jnp.int32)
    return ((cell_x * CY + cell_y) * CZ + cell_z).astype(jnp.int32)


def draw_inverse(key, part):
    shape = (DEVICES, N_GRP, CAP, SEGB, SEGB)
    noise_key = jax.random.fold_in(key, 15)
    spread = 1.0 / math.sqrt(SEGB)
    noise = spread * jnp.clip(jax.random.normal(noise_key, shape, jnp.float32), -4.0, 4.0)
    return jnp.eye(SEGB, dtype=jnp.float32) + noise


def place_ends(values, stream_key, low, largest):
    dims = values.shape
    spot = [jax.random.randint(jax.random.fold_in(stream_key, axis), (), 0, dims[axis]) for axis in range(len(dims))]
    values = values.at[tuple(spot)].set(low)
    longest = dims.index(max(dims))
    spot[longest] = (spot[longest] + 1) % dims[longest]
    return values.at[tuple(spot)].set(largest)


def levels(stream_key, shape, pieces, low, largest):
    factor_of, own = 1.0, jax.random.fold_in(stream_key, 6)
    for axis_at, blocks in pieces:
        heights = jnp.exp(jax.random.uniform(jax.random.fold_in(own, axis_at), (blocks,), jnp.float32, low / len(pieces), largest / len(pieces)))
        factor_of = factor_of * jnp.repeat(heights, shape[axis_at] // blocks).reshape([-1 if axis == axis_at else 1 for axis in range(len(shape))])
    return factor_of


def shared_out(rng, own, number, rows, number_of, top, bound, slope):
    ranking = jax.random.permutation(rng, number_of)
    heavy_load, ordinary = load_shares(number_of, rows * top, bound, slope, True), load_shares(number_of, rows * top, bound, slope, False)
    places = jnp.arange(number_of)

    def named(lengths, rotation):
        used = int((lengths > 0).sum())
        fixed = max(1, used // 4)
        shifted = fixed + (places - fixed + rotation * (used - fixed)) % max(1, number_of - fixed)
        return jnp.zeros((number_of,), jnp.int32).at[ranking[jnp.where(places < fixed, places, shifted)]].set(jnp.asarray(lengths, jnp.int32))

    lengths = jnp.where(number % 4 == 0, named(heavy_load, number // 4), named(ordinary, number - number // 4 - 1))
    mixed = jax.random.permutation(jax.random.fold_in(own, 3), number_of)
    donor, taker = mixed[0:number_of // 2 * 2:2], mixed[1:number_of // 2 * 2:2]
    margin = jnp.minimum(lengths[donor] - 1, bound - lengths[taker]) // 2
    margin = jnp.where((donor == ranking[0]) | (taker == ranking[0]) | (lengths[taker] == 0), 0, jnp.maximum(margin, 0))
    shifted = jax.random.randint(jax.random.fold_in(own, 4), (number_of // 2,), 0, 1 << 20) % (margin + 1)
    lengths = lengths.at[donor].add(-shifted).at[taker].add(shifted)
    labels = jnp.searchsorted(jnp.cumsum(lengths), jnp.arange(rows * top), side="right").astype(jnp.int32)
    listing = labels.reshape(top, rows).T
    listing = listing[jax.random.permutation(jax.random.fold_in(own, 1), rows)]
    rotation = jax.random.randint(jax.random.fold_in(own, 2), (rows, 1), 0, top)
    return jnp.take_along_axis(listing, (jnp.arange(top)[None, :] + rotation) % top, axis=1)


def load_shares(count, total, most, lean, full):
    loads = [(1 << 20) // math.isqrt(rank ** lean) + 1 for rank in range(1, count + 1)]
    largest = most if full else min(most, max(-(-total // count), total * loads[0] // sum(loads)))
    least = 1 if total - largest >= count - 1 else 0
    counts, spare = [largest] + [least] * (count - 1), total - largest - least * (count - 1)
    while spare > 0:
        candidates = [i for i in range(1, count) if counts[i] < largest] or [i for i in range(1, count) if counts[i] < most]
        pool, left = sum([loads[i] for i in candidates]), spare
        for i in candidates:
            extra = min(most - counts[i], max(1, left * loads[i] // pool), spare)
            counts[i] = counts[i] + extra
            spare = spare - extra
    return np.array(counts)


def normal_values(key, shape, width, bound, pieces=(), kind=jnp.bfloat16):
    entries = jax.random.normal(key, shape, jnp.float32) * width
    if len(pieces) > 0:
        entries = levels(key, shape, pieces, -0.22, 0.18) * entries
    return jnp.clip(entries, min=-bound, max=bound).astype(kind)


def setup_inputs(seed: int = 0) -> dict:
    key_list = jax.random.split(jax.random.key(seed), 10)
    right_side = draw_right_side(jax.random.fold_in(key_list[9], 71), 0)
    accumulation = draw_accumulation(jax.random.fold_in(key_list[9], 71), 0)
    transmissibility = draw_transmissibility(jax.random.fold_in(key_list[9], 71), 0)
    completion = draw_completion(jax.random.fold_in(key_list[9], 71), 0)
    live_count = place_ends(jax.random.randint(key_list[4], (NBLK,), SEGB // 4, SEGB + 1), jax.random.fold_in(key_list[4], 1), SEGB // 4, SEGB).astype(jnp.int32)
    owner_keys = jax.random.split(jax.random.fold_in(key_list[5], 1), NBLK // BH)
    owner_turns = jax.random.permutation(jax.random.fold_in(key_list[5], 3), NBLK // BH)
    owner = jax.vmap(lambda own, number: shared_out(jax.random.fold_in(key_list[5], 2), own, number, BH, N_GRP, 1, CAP, 2))(owner_keys, owner_turns).reshape((NBLK, 1))
    cell_to_well = normal_values(key_list[6], (NBLK, COMP, SEGB), 1.0, 3.0, ((0, 128),), jnp.float32)
    well_to_cell = normal_values(key_list[7], (NBLK, COMP, SEGB), 1.0, 3.0, ((0, 128),), jnp.float32)
    inverse = draw_inverse(jax.random.fold_in(key_list[9], 71), 0)
    return {"right_side": right_side, "accumulation": accumulation, "transmissibility": transmissibility, "completion": completion, "live_count": live_count, "owner": owner, "cell_to_well": cell_to_well, "well_to_cell": well_to_cell, "inverse": inverse}


def stencil(vector, diag_total, transmissibility):
    padded = jnp.pad(vector, ((0, 0), (1, 1), (1, 1), (1, 1)))
    beside_list = [padded[:, 2:, 1:-1, 1:-1], padded[:, :-2, 1:-1, 1:-1],
                   padded[:, 1:-1, 2:, 1:-1], padded[:, 1:-1, :-2, 1:-1],
                   padded[:, 1:-1, 1:-1, 2:], padded[:, 1:-1, 1:-1, :-2]]
    result = jnp.sum(diag_total * vector[None], axis=1)
    for face in range(6):
        result = result - jnp.sum(transmissibility[face] * beside_list[face][None], axis=1)
    return result


def reference(right_side, accumulation, transmissibility, completion, live_count, owner, cell_to_well, well_to_cell, inverse):
    diag_total = accumulation
    for face in range(6):
        diag_total = diag_total + transmissibility[face]
    owner_col = owner[:, 0]
    device_of = jnp.arange(NBLK, dtype=jnp.int32) // BH
    home_grp = device_of % N_GRP
    home_res = device_of // N_GRP
    owner_eq = (owner_col[:, None] == jnp.arange(N_GRP, dtype=jnp.int32)[None, :]).astype(jnp.int32)
    owner_eq = owner_eq.reshape(N_RES * N_GRP, BH, N_GRP)
    prior = jnp.cumsum(owner_eq, axis=1) - owner_eq
    slot_number = jnp.sum(prior * owner_eq, axis=2).reshape(-1).astype(jnp.int32)
    block_inverse = inverse[home_res * N_GRP + owner_col, home_grp, slot_number]
    segb = completion.shape[1]
    open_mask = (jnp.arange(segb, dtype=jnp.int32)[None, :] < live_count[:, None]).astype(jnp.float32)
    local_x = completion // (CY * CZ)
    local_y = (completion // CZ) % CY
    local_z = completion % CZ
    global_x = home_res[:, None] * CX + local_x
    global_y = home_grp[:, None] * CY + local_y
    flat_index = ((global_x * NY + global_y) * NZ + local_z).reshape(-1).astype(jnp.int32)

    def operator(vector):
        result = stencil(vector, diag_total, transmissibility)
        flat = vector.reshape(COMP, -1)
        picked = jnp.moveaxis(flat[:, flat_index].reshape(COMP, NBLK, segb), 0, 1)
        coupled = jnp.sum(cell_to_well * picked, axis=1) * open_mask
        well_value = jnp.einsum("bst,bt->bs", block_inverse, coupled, precision=lax.Precision.HIGHEST)
        correction = well_to_cell * (well_value * open_mask)[:, None, :]
        correction = jnp.moveaxis(correction, 0, 1).reshape(COMP, -1)
        out_flat = result.reshape(COMP, -1).at[:, flat_index].add(-correction)
        return out_flat.reshape(vector.shape)

    solution = jnp.zeros_like(right_side)
    residual = right_side
    shadow = right_side
    search = right_side
    rho = jnp.sum(residual * residual)
    for index in range(ITERS):
        image = operator(search)
        alpha = rho / jnp.sum(shadow * image)
        middle = residual - alpha * image
        second = operator(middle)
        omega = jnp.sum(second * middle) / jnp.sum(second * second)
        solution = solution + alpha * search + omega * middle
        residual = middle - omega * second
        if index + 1 < ITERS:
            rho_next = jnp.sum(shadow * residual)
            search = residual + (rho_next / rho) * (alpha / omega) * (search - omega * image)
            rho = rho_next
    return solution, residual
```

```python
import functools

import jax
import jax.numpy as jnp
from jax import lax
from jax.experimental import pallas as pl
from jax.experimental.pallas import tpu as pltpu
from jax.sharding import PartitionSpec as P

ITERS = 3
RES_GRP = ("res", "grp")
MESH = pl.DeviceIdType.MESH
F32, BF16 = jnp.float32, jnp.bfloat16
R0, R, W, T, PP, S, Z, V, X, Q, Y = range(11)


def kernel(
    n_res,
    n_grp,
    live_ref,
    owner_ref,
    rhs_hbm,
    acc_hbm,
    trans_hbm,
    comp_hbm,
    c2w_hbm,
    w2c_hbm,
    inv_hbm,
    x_out,
    r_out,
    fld,
    diag,
    trans,
    inv,
    comp,
    c2w,
    w2c,
    picks,
    spread,
    hot,
    grid_of,
    lhs,
    xs,
    hx,
    hy,
    ysend,
    csend,
    crecv,
    vsend,
    vrecv,
    rsend,
    rrecv,
    scal,
    in_sem,
    hx_ss,
    hx_rs,
    hy_ss,
    hy_rs,
    c_ss,
    c_rs,
    v_ss,
    v_rs,
    r_ss,
    r_rs,
    out_sem,
):
    n_dev = n_res * n_grp
    r, g = lax.axis_index("res"), lax.axis_index("grp")
    me = r * n_grp + g

    def load(i, src, dst):
        return pltpu.make_async_copy(src, dst, in_sem.at[i])

    loads = [
        load(0, comp_hbm, comp),
        load(1, c2w_hbm, c2w),
        load(2, w2c_hbm, w2c),
        load(3, rhs_hbm, fld.at[R0]),
        load(4, acc_hbm, diag),
    ]
    loads += [load(5 + f, trans_hbm.at[f], trans.at[f]) for f in range(6)]
    loads += [load(11 + h, inv_hbm.at[0, h], inv.at[h]) for h in range(4)]
    for copy in loads:
        copy.start()

    hx[...] = jnp.zeros_like(hx)
    hy[...] = jnp.zeros_like(hy)

    barrier = pltpu.get_barrier_semaphore()

    def peer(k):
        other = lax.rem(me + k, n_dev)
        return (lax.div(other, n_grp), lax.rem(other, n_grp))

    def greet(k, carry):
        pl.semaphore_signal(barrier, inc=1, device_id=peer(k), device_id_type=MESH)
        return carry

    lax.fori_loop(1, n_dev, greet, 0)

    for field in (PP, S, Z, V, X):
        fld[field] = jnp.zeros((3, 2, 16, 512), F32)
    scal[...] = jnp.ones_like(scal)
    csend[...] = jnp.zeros_like(csend)
    ysend[...] = jnp.zeros_like(ysend)

    owners = [owner_ref[b, 0] for b in range(8)]
    target = []
    for b in range(8):
        slot = jnp.int32(0)
        for a in range(b):
            slot = slot + jnp.where(owners[a] == owners[b], 1, 0).astype(jnp.int32)
        target.append(lax.rem(owners[b] - g + n_grp, n_grp) * 8 + slot)

    for copy in loads[:3]:
        copy.wait()
    seg = lax.broadcasted_iota(jnp.int32, (1, 256), 1)
    for b in range(8):
        opened = seg < live_ref[b]
        c2w[b] = jnp.where(opened, c2w[b], 0.0)
        w2c[b] = jnp.where(opened, w2c[b], 0.0)
        cell = comp[b : b + 1, :]
        low = cell & 255
        half = (cell >> 8) & 1
        high = cell >> 9
        one = jnp.where(lax.broadcasted_iota(jnp.int32, (256, 256), 0) == low, 1.0, 0.0).astype(F32)
        picks[b] = one.astype(BF16)
        spread[b * 256 : (b + 1) * 256, :] = jnp.transpose(one).astype(BF16)
        rows = lax.broadcasted_iota(jnp.int32, (32, 256), 0)
        for zh in range(2):
            here = (rows == high) & (half == zh)
            hot[b, zh] = jnp.where(here, 1.0, 0.0).astype(BF16)
            for i in range(3):
                grid_of[b, zh * 96 + i * 32 : zh * 96 + (i + 1) * 32, :] = jnp.where(
                    here, c2w[b, i : i + 1, :], 0.0
                )

    for copy in loads[3:11]:
        copy.wait()
    for x in range(2):
        for i in range(3):
            for j in range(3):
                total = diag[i, j, x]
                for f in range(6):
                    total = total + trans[f, i, j, x]
                diag[i, j, x] = total
    for i in range(3):
        fld[R, i] = fld[R0, i]
    for copy in loads[11:]:
        copy.wait()

    pl.semaphore_wait(barrier, n_dev - 1)

    def remote(src, dst, ss, rs, device):
        return pltpu.make_async_remote_copy(
            src_ref=src, dst_ref=dst, send_sem=ss, recv_sem=rs, device_id=device, device_id_type=MESH
        )

    lane512 = lax.broadcasted_iota(jnp.int32, (8, 512), 1)
    row8 = lax.broadcasted_iota(jnp.int32, (8, 512), 0)
    iota32 = lax.broadcasted_iota(jnp.int32, (32, 256), 0)
    lane = lax.broadcasted_iota(jnp.int32, (1, 128), 1)

    def spmv(src, dst, par):
        x_up = remote(fld.at[src, :, 1], hx.at[par, 0], hx_ss.at[0], hx_rs.at[par, 0], (r + 1, g))
        x_dn = remote(fld.at[src, :, 0], hx.at[par, 1], hx_ss.at[1], hx_rs.at[par, 1], (r - 1, g))
        y_up = remote(ysend.at[0], hy.at[par, 0], hy_ss.at[0], hy_rs.at[par, 0], (r, g + 1))
        y_dn = remote(ysend.at[1], hy.at[par, 1], hy_ss.at[1], hy_rs.at[par, 1], (r, g - 1))
        pl.when(r < n_res - 1)(x_up.start)
        pl.when(r > 0)(x_dn.start)
        for j in range(3):
            for x in range(2):
                at = j * 2 + x
                ysend[0, at : at + 1, :] = fld[src, j, x, 15:16, :]
                ysend[1, at : at + 1, :] = fld[src, j, x, 0:1, :]
        pl.when(g < n_grp - 1)(y_up.start)
        pl.when(g > 0)(y_dn.start)

        for zh in range(2):
            v = fld[src, :, :, :, zh * 256 : (zh + 1) * 256].reshape(96, 256)
            top = v.astype(BF16)
            lhs[zh * 96 : (zh + 1) * 96, :] = top
            lhs[192 + zh * 96 : 192 + (zh + 1) * 96, :] = (v - top.astype(F32)).astype(BF16)
        out = jnp.zeros((32, 256), F32)
        for b in range(8):
            got = jnp.dot(lhs[...], picks[b], preferred_element_type=F32)
            row = jnp.sum((got[:192] + got[192:]) * grid_of[b], axis=0, keepdims=True)
            out = jnp.where(iota32 == target[b], row, out)
        csend[...] = out.reshape(4, 8, 256)
        c_copies = {}
        for d in (2, 1, 3):
            to = (r, lax.rem(g + d, n_grp))
            c_copies[d] = remote(csend.at[d], crecv.at[par, 4 - d], c_ss.at[d], c_rs.at[par, 4 - d], to)
            c_copies[d].start()

        for x in range(2):
            for yt in range(2):
                ys = slice(yt * 8, yt * 8 + 8)
                sums = [None] * 3
                for j in range(3):
                    v = fld[src, j, x, ys, :]
                    zp = jnp.where(lane512 == 511, 0.0, pltpu.roll(v, 511, 1))
                    zm = jnp.where(lane512 == 0, 0.0, pltpu.roll(v, 1, 1))
                    if yt == 0:
                        yp = fld[src, j, x, 1:9, :]
                        ym = jnp.where(row8 == 0, 0.0, pltpu.roll(v, 1, 0))
                    else:
                        yp = jnp.where(row8 == 7, 0.0, pltpu.roll(v, 7, 0))
                        ym = fld[src, j, x, 7:15, :]
                    xn = fld[src, j, 1 - x, ys, :]
                    for i in range(3):
                        part = diag[i, j, x, ys, :] * v
                        part = part - trans[x, i, j, x, ys, :] * xn
                        part = part - trans[2, i, j, x, ys, :] * yp
                        part = part - trans[3, i, j, x, ys, :] * ym
                        part = part - trans[4, i, j, x, ys, :] * zp
                        part = part - trans[5, i, j, x, ys, :] * zm
                        sums[i] = part if sums[i] is None else sums[i] + part
                for i in range(3):
                    fld[dst, i, x, ys, :] = sums[i]

        lane128 = lax.broadcasted_iota(jnp.int32, (256, 128), 1)
        v_copies = {}
        for d in (0, 1, 3, 2):
            home = lax.rem(g + d, n_grp)
            if d == 0:
                c8 = csend[0]
            else:
                remote(csend.at[d], crecv.at[par, d], c_ss.at[d], c_rs.at[par, d], (r, home)).wait_recv()
                c8 = crecv[par, d]
            columns = jnp.zeros((256, 128), F32)
            for k in range(4):
                column = jnp.sum(inv[home, k] * c8[k : k + 1, :], axis=1, keepdims=True)
                columns = jnp.where(lane128 == k, column, columns)
            values = jnp.transpose(columns)[0:8]
            if d == 0:
                vrecv[par, 0] = values
            else:
                vsend[d] = values
                v_copies[d] = remote(
                    vsend.at[d], vrecv.at[par, 4 - d], v_ss.at[d], v_rs.at[par, 4 - d], (r, home)
                )
                v_copies[d].start()

        pl.when(r > 0)(x_up.wait_recv)
        pl.when(r < n_res - 1)(x_dn.wait_recv)
        pl.when(g > 0)(y_up.wait_recv)
        pl.when(g < n_grp - 1)(y_dn.wait_recv)
        for x in range(2):
            side, face = (0, 1) if x == 0 else (1, 0)
            for i in range(3):
                part = trans[face, i, 0, x] * hx[par, side, 0]
                for j in range(1, 3):
                    part = part + trans[face, i, j, x] * hx[par, side, j]
                low_y = trans[3, i, 0, x, 0:8, :] * hy[par, 0, x : x + 1, :]
                high_y = trans[2, i, 0, x, 8:16, :] * hy[par, 1, x : x + 1, :]
                for j in range(1, 3):
                    at = slice(j * 2 + x, j * 2 + x + 1)
                    low_y = low_y + trans[3, i, j, x, 0:8, :] * hy[par, 0, at, :]
                    high_y = high_y + trans[2, i, j, x, 8:16, :] * hy[par, 1, at, :]
                low = fld[dst, i, x, 0:8, :] - part[0:8]
                fld[dst, i, x, 0:8, :] = low - jnp.where(row8 == 0, low_y, 0.0)
                high = fld[dst, i, x, 8:16, :] - part[8:16]
                fld[dst, i, x, 8:16, :] = high - jnp.where(row8 == 7, high_y, 0.0)

        for d in (1, 3, 2):
            remote(vsend.at[d], vrecv.at[par, d], v_ss.at[d], v_rs.at[par, d], (r, g)).wait_recv()
        back = vrecv[par].reshape(32, 256)
        for b in range(8):
            value = jnp.sum(jnp.where(iota32 == target[b], back, 0.0), axis=0, keepdims=True)
            for i in range(3):
                term = jnp.broadcast_to(w2c[b, i : i + 1, :] * value, (32, 256))
                top = term.astype(BF16)
                rest = (term - top.astype(F32)).astype(BF16)
                for zh in range(2):
                    at = zh * 96 + i * 32
                    xs[at : at + 32, b * 256 : (b + 1) * 256] = hot[b, zh] * top
                    xs[192 + at : 192 + at + 32, b * 256 : (b + 1) * 256] = hot[b, zh] * rest
        got = jnp.dot(xs[...], spread[...], preferred_element_type=F32)
        got = got[:192] + got[192:]
        for zh in range(2):
            for i in range(3):
                for x in range(2):
                    at = zh * 96 + i * 32 + x * 16
                    zs = slice(zh * 256, (zh + 1) * 256)
                    fld[dst, i, x, :, zs] = fld[dst, i, x, :, zs] - got[at : at + 16]

        pl.when(r < n_res - 1)(x_up.wait_send)
        pl.when(r > 0)(x_dn.wait_send)
        pl.when(g < n_grp - 1)(y_up.wait_send)
        pl.when(g > 0)(y_dn.wait_send)
        for d in (1, 2, 3):
            c_copies[d].wait_send()
            v_copies[d].wait_send()

    def fold(block):
        half = block[0:8] + block[8:16]
        return (half[:, 0:128] + half[:, 128:256]) + (half[:, 256:384] + half[:, 384:512])

    def sums_start(pairs, par):
        row = jnp.zeros((1, 128), F32)
        for k, (a, b) in enumerate(pairs):
            total = jnp.zeros((8, 128), F32)
            for i in range(3):
                for x in range(2):
                    total = total + fold(fld[a, i, x] * fld[b, i, x])
            one = jnp.sum(jnp.sum(total, axis=0, keepdims=True), axis=1, keepdims=True)
            row = jnp.where(lane == k, one, row)
        rsend[0] = row
        rrecv[par, me] = row

        def send(k, carry):
            remote(rsend, rrecv.at[par, pl.ds(me, 1)], r_ss, r_rs.at[par], peer(k)).start()
            return carry

        lax.fori_loop(1, n_dev, send, 0)

    def sums_wait(par):
        some = rrecv.at[par, pl.ds(0, n_dev - 1)]
        pltpu.make_async_copy(some, some, r_rs.at[par]).wait()
        pltpu.make_async_copy(some, some, r_ss).wait()
        row = jnp.sum(rrecv[par], axis=0)
        return [
            jnp.sum(jnp.where(lane == k, row, 0.0), axis=1, keepdims=True) for k in range(4)
        ]

    def keep(at, value):
        scal[at] = jnp.broadcast_to(value, (8, 128))

    def kept(at):
        return scal[at, 0:1, 0:1]

    def wide(value):
        return jnp.broadcast_to(value, (16, 512))

    RHO, ALPHA, OMEGA = 0, 1, 2

    def middle_step(par):
        inner, square, _, _ = sums_wait(par)
        omega = inner / square
        keep(OMEGA, omega)
        om, al = wide(omega), wide(kept(ALPHA))
        return om, al

    def step(j, carry):
        par = lax.rem(j, 2)
        odd = par == 1
        first = j == 0
        src = jnp.where(odd, W, jnp.where(first, R, Z))
        dst = jnp.where(odd, T, jnp.where(first, W, V))
        spmv(src, dst, par)

        @pl.when(jnp.logical_not(odd))
        def _():
            @pl.when(j > 0)
            def _():
                om, al = middle_step(1 - par)
                for i in range(3):
                    for x in range(2):
                        q, y = fld[Q, i, x], fld[Y, i, x]
                        fld[X, i, x] = fld[X, i, x] + al * fld[PP, i, x] + om * q
                        fld[R, i, x] = q - om * y
                        fld[W, i, x] = y - om * (fld[T, i, x] - al * fld[V, i, x])

            sums_start([(R0, R), (R0, W), (R0, S), (R0, Z)], par)

        @pl.when(odd)
        def _():
            rho_next, along_w, along_s, along_z = sums_wait(1 - par)
            omega = kept(OMEGA)
            beta = rho_next / kept(RHO) * (kept(ALPHA) / omega)
            beta = jnp.where(j == 1, 0.0, beta)
            alpha = rho_next / (along_w + beta * (along_s - omega * along_z))
            keep(RHO, rho_next)
            keep(ALPHA, alpha)
            be, om, al = wide(beta), wide(omega), wide(alpha)
            for i in range(3):
                for x in range(2):
                    s, z = fld[S, i, x], fld[Z, i, x]
                    res, w = fld[R, i, x], fld[W, i, x]
                    fld[PP, i, x] = res + be * (fld[PP, i, x] - om * s)
                    s = w + be * (s - om * z)
                    z = fld[T, i, x] + be * (z - om * fld[V, i, x])
                    fld[S, i, x] = s
                    fld[Z, i, x] = z
                    fld[Q, i, x] = res - al * s
                    fld[Y, i, x] = w - al * z
            sums_start([(Q, Y), (Y, Y)], par)

        return carry

    lax.fori_loop(0, 2 * ITERS, step, 0)
    om, al = middle_step(1)
    for i in range(3):
        for x in range(2):
            q = fld[Q, i, x]
            fld[X, i, x] = fld[X, i, x] + al * fld[PP, i, x] + om * q
            fld[R, i, x] = q - om * fld[Y, i, x]
    outs = [
        pltpu.make_async_copy(fld.at[X], x_out, out_sem.at[0]),
        pltpu.make_async_copy(fld.at[R], r_out, out_sem.at[1]),
    ]
    for copy in outs:
        copy.start()
    for copy in outs:
        copy.wait()


def solution(mesh):
    n_res, n_grp = mesh.shape["res"], mesh.shape["grp"]
    n_dev = n_res * n_grp

    def body(right_side, accumulation, transmissibility, completion, live_count, owner, c2w, w2c, inverse):
        dma = pltpu.SemaphoreType.DMA
        field = (3, 2, 16, 512)
        any_space = pl.BlockSpec(memory_space=pl.ANY)
        smem = pl.BlockSpec(memory_space=pltpu.SMEM)
        return pl.pallas_call(
            functools.partial(kernel, n_res, n_grp),
            name="bicgstab",
            out_shape=[jax.ShapeDtypeStruct(field, F32)] * 2,
            in_specs=[smem, smem] + [any_space] * 7,
            out_specs=[any_space] * 2,
            scratch_shapes=[
                pltpu.VMEM((11,) + field, F32),
                pltpu.VMEM((3, 3, 2, 16, 512), F32),
                pltpu.VMEM((6, 3, 3, 2, 16, 512), F32),
                pltpu.VMEM((4, 4, 256, 256), F32),
                pltpu.VMEM((8, 256), jnp.int32),
                pltpu.VMEM((8, 3, 256), F32),
                pltpu.VMEM((8, 3, 256), F32),
                pltpu.VMEM((8, 256, 256), BF16),
                pltpu.VMEM((2048, 256), BF16),
                pltpu.VMEM((8, 2, 32, 256), BF16),
                pltpu.VMEM((8, 192, 256), F32),
                pltpu.VMEM((384, 256), BF16),
                pltpu.VMEM((384, 2048), BF16),
                pltpu.VMEM((2, 2, 3, 16, 512), F32),
                pltpu.VMEM((2, 2, 8, 512), F32),
                pltpu.VMEM((2, 8, 512), F32),
                pltpu.VMEM((4, 8, 256), F32),
                pltpu.VMEM((2, 4, 8, 256), F32),
                pltpu.VMEM((4, 8, 256), F32),
                pltpu.VMEM((2, 4, 8, 256), F32),
                pltpu.VMEM((1, 1, 128), F32),
                pltpu.VMEM((2, n_dev, 1, 128), F32),
                pltpu.VMEM((4, 8, 128), F32),
                dma((15,)),
                dma((2,)),
                dma((2, 2)),
                dma((2,)),
                dma((2, 2)),
                dma((4,)),
                dma((2, 4)),
                dma((4,)),
                dma((2, 4)),
                dma(()),
                dma((2,)),
                dma((2,)),
            ],
            compiler_params=pltpu.CompilerParams(collective_id=0, has_side_effects=True),
        )(live_count, owner, right_side, accumulation, transmissibility, completion, c2w, w2c, inverse)

    in_specs = (
        P(None, "res", "grp", None),
        P(None, None, "res", "grp", None),
        P(None, None, None, "res", "grp", None),
        P(RES_GRP, None),
        P(RES_GRP),
        P(RES_GRP, None),
        P(RES_GRP, None, None),
        P(RES_GRP, None, None),
        P(RES_GRP, None, None, None, None),
    )
    out_specs = (P(None, "res", "grp", None), P(None, "res", "grp", None))

    def run(*args):
        first, second = jax.shard_map(
            body, mesh=mesh, in_specs=in_specs, out_specs=out_specs, check_vma=False
        )(*args)
        return first, second

    return run
```

```python
import functools

import jax
import jax.numpy as jnp
from jax import lax
from jax.experimental import pallas as pl
from jax.experimental.pallas import tpu as pltpu
from jax.sharding import PartitionSpec as P

ITERS = 3
RES_GRP = ("res", "grp")
MESH, LOGICAL = pl.DeviceIdType.MESH, pl.DeviceIdType.LOGICAL
F32, BF16 = jnp.float32, jnp.bfloat16
R0, R, W, T, PP, S, Z, V, X, Q, Y, SPARE = range(12)


def kernel(
    n_res,
    n_grp,
    live_hbm,
    owner_hbm,
    rhs_hbm,
    acc_hbm,
    trans_hbm,
    comp_hbm,
    c2w_hbm,
    w2c_hbm,
    inv_hbm,
    x_out,
    r_out,
    live,
    owner,
    fld,
    diag,
    trans,
    inv,
    comp,
    c2w,
    w2c,
    picks,
    spread,
    hot,
    grid_of,
    lhs,
    xs,
    hx,
    hy,
    ysend,
    csend,
    crecv,
    vsend,
    vrecv,
    rsend,
    rrecv,
    scal,
    in_sem,
    hx_ss,
    hx_rs,
    hy_ss,
    hy_rs,
    c_ss,
    c_rs,
    v_ss,
    v_rs,
    r_ss,
    r_rs,
    out_sem,
):
    n_dev = n_res * n_grp
    r, g = lax.axis_index("res"), lax.axis_index("grp")
    me = r * n_grp + g

    def load(i, src, dst):
        return pltpu.make_async_copy(src, dst, in_sem.at[i])

    first_loads = [
        load(0, comp_hbm, comp),
        load(1, live_hbm, live),
        load(2, owner_hbm, owner),
        load(3, c2w_hbm, c2w),
        load(4, w2c_hbm, w2c),
        load(5, rhs_hbm, fld.at[R0]),
        load(6, rhs_hbm, fld.at[R]),
    ]
    face_loads = [load(7, acc_hbm, diag)] + [load(8 + f, trans_hbm.at[f], trans.at[f]) for f in range(6)]
    inverse_loads = [load(14 + h, inv_hbm.at[0, h], inv.at[h]) for h in range(4)]
    for copy in first_loads + face_loads + inverse_loads:
        copy.start()

    hx[...] = jnp.zeros_like(hx)
    hy[...] = jnp.zeros_like(hy)
    rrecv[...] = jnp.zeros_like(rrecv)

    barrier = pltpu.get_barrier_semaphore()

    def peer(k):
        return (me + k) & (n_dev - 1)

    def greet(k, carry):
        pl.semaphore_signal(barrier, inc=1, device_id=peer(k), device_id_type=LOGICAL)
        return carry

    lax.fori_loop(1, n_dev, greet, 0)

    for field in (T, PP, S, Z, V, X, Y):
        fld[field] = jnp.zeros((3, 2, 16, 512), F32)
    scal[...] = jnp.ones_like(scal)
    csend[...] = jnp.zeros_like(csend)
    ysend[...] = jnp.zeros_like(ysend)

    for copy in first_loads[:5]:
        copy.wait()
    owners = [owner[0, b] for b in range(8)]
    target = []
    for b in range(8):
        slot = jnp.int32(0)
        for a in range(b):
            slot = slot + jnp.where(owners[a] == owners[b], 1, 0).astype(jnp.int32)
        target.append(((owners[b] - g) & (n_grp - 1)) * 4 + slot)

    seg = lax.broadcasted_iota(jnp.int32, (8, 256), 1)
    well = lax.broadcasted_iota(jnp.int32, (8, 256), 0)
    lives = jnp.zeros((8, 256), jnp.int32)
    for b in range(8):
        lives = jnp.where(well == b, live[b], lives)
    for i in range(3):
        c2w[i] = jnp.where(seg < lives, c2w[i], 0.0)
        w2c[i] = jnp.where(seg < lives, w2c[i], 0.0)
    for b in range(8):
        cell = comp[b : b + 1, :]
        low = cell & 255
        half = (cell >> 8) & 1
        high = cell >> 9
        one = jnp.where(lax.broadcasted_iota(jnp.int32, (256, 256), 0) == low, 1.0, 0.0).astype(F32)
        picks[b] = one.astype(BF16)
        spread[b * 256 : (b + 1) * 256, :] = jnp.transpose(one).astype(BF16)
        rows = lax.broadcasted_iota(jnp.int32, (32, 256), 0)
        for zh in range(2):
            here = (rows == high) & (half == zh)
            hot[b, zh] = jnp.where(here, 1.0, 0.0).astype(BF16)
            for i in range(3):
                grid_of[b, zh * 96 + i * 32 : zh * 96 + (i + 1) * 32, :] = jnp.where(
                    here, c2w[i, b : b + 1, :], 0.0
                )
    for copy in first_loads[5:]:
        copy.wait()

    def remote(src, dst, ss, rs, device):
        return pltpu.make_async_remote_copy(
            src_ref=src, dst_ref=dst, send_sem=ss, recv_sem=rs, device_id=device, device_id_type=MESH
        )

    lane512 = lax.broadcasted_iota(jnp.int32, (8, 512), 1)
    row8 = lax.broadcasted_iota(jnp.int32, (8, 512), 0)
    iota4 = lax.broadcasted_iota(jnp.int32, (4, 256), 0)
    iota16 = lax.broadcasted_iota(jnp.int32, (16, 256), 0)
    lane = lax.broadcasted_iota(jnp.int32, (1, 128), 1)
    RHO, ALPHA, OMEGA, BETA = 0, 1, 2, 3

    def keep(at, value):
        scal[at] = jnp.broadcast_to(value, (8, 128))

    def kept(at):
        return scal[at, 0:1, 0:1]

    def wide(value):
        return jnp.broadcast_to(value, (16, 512))

    def fold(block):
        half = block[0:8] + block[8:16]
        return (half[:, 0:128] + half[:, 128:256]) + (half[:, 256:384] + half[:, 384:512])

    def sums_start(totals, par):
        row = jnp.zeros((1, 128), F32)
        for k, total in enumerate(totals):
            one = jnp.sum(jnp.sum(total, axis=0, keepdims=True), axis=1, keepdims=True)
            row = jnp.where(lane == k, one, row)
        rsend[0] = row
        rrecv[par, me] = row

        def send(k, carry):
            pltpu.make_async_remote_copy(
                src_ref=rsend,
                dst_ref=rrecv.at[par, pl.ds(me, 1)],
                send_sem=r_ss,
                recv_sem=r_rs.at[par],
                device_id=peer(k),
                device_id_type=LOGICAL,
            ).start()
            return carry

        lax.fori_loop(1, n_dev, send, 0)

    def sums_wait(par):
        some = rrecv.at[par, pl.ds(0, n_dev - 1)]
        pltpu.make_async_copy(some, some, r_rs.at[par]).wait()
        pltpu.make_async_copy(some, some, r_ss).wait()

    def sums_of(par):
        row = jnp.sum(rrecv[par], axis=0)
        return [jnp.sum(jnp.where(lane == k, row, 0.0), axis=1, keepdims=True) for k in range(4)]

    tiles = [(i, x) for i in range(3) for x in range(2)]

    def odd_rest(par):
        be, om, al = wide(kept(BETA)), wide(kept(OMEGA)), wide(kept(ALPHA))
        inner, square = jnp.zeros((8, 128), F32), jnp.zeros((8, 128), F32)
        for i, x in tiles:
            s, res, w = fld[S, i, x], fld[R, i, x], fld[W, i, x]
            fld[PP, i, x] = res + be * (fld[PP, i, x] - om * s)
            s = w + be * (s - om * fld[Q, i, x])
            fld[S, i, x] = s
            q = res - al * s
            y = w - al * fld[Z, i, x]
            fld[Q, i, x] = q
            fld[Y, i, x] = y
            inner = inner + fold(q * y)
            square = square + fold(y * y)
        sums_start([inner, square], par)

    def step(j, carry):
        par = j & 1
        odd = par == 1
        first = j == 0
        src = jnp.where(odd, W, jnp.where(first, R, Z))
        dst = jnp.where(odd, T, jnp.where(first, W, V))

        for zh in range(2):
            v = fld[src, :, :, :, zh * 256 : (zh + 1) * 256].reshape(96, 256)
            top = v.astype(BF16)
            lhs[zh * 96 : (zh + 1) * 96, :] = top
            lhs[192 + zh * 96 : 192 + (zh + 1) * 96, :] = (v - top.astype(F32)).astype(BF16)
        out = jnp.zeros((16, 256), F32)
        for b in range(8):
            got = jnp.dot(lhs[...], picks[b], preferred_element_type=F32)
            row = jnp.sum((got[:192] + got[192:]) * grid_of[b], axis=0, keepdims=True)
            out = jnp.where(iota16 == target[b], row, out)
        for d in range(4):
            csend[d] = out[d * 4 : (d + 1) * 4]
        for k in range(2):
            for x in range(2):
                for j3 in range(3):
                    at = j3 * 2 + x
                    edge = 15 if k == 0 else 0
                    ysend[k, at : at + 1, :] = fld[src, j3, x, edge : edge + 1, :]

        @pl.when(first)
        def _():
            pl.semaphore_wait(barrier, n_dev - 1)

        c_copies = {}
        for d in (2, 1, 3):
            to = (r, (g + d) & (n_grp - 1))
            c_copies[d] = remote(csend.at[d], crecv.at[par, 4 - d], c_ss.at[d], c_rs.at[par, 4 - d], to)
            c_copies[d].start()

        x_up = remote(fld.at[src, :, 1], hx.at[par, 0], hx_ss.at[0], hx_rs.at[par, 0], (r + 1, g))
        x_dn = remote(fld.at[src, :, 0], hx.at[par, 1], hx_ss.at[1], hx_rs.at[par, 1], (r - 1, g))
        y_up = remote(ysend.at[0], hy.at[par, 0], hy_ss.at[0], hy_rs.at[par, 0], (r, g + 1))
        y_dn = remote(ysend.at[1], hy.at[par, 1], hy_ss.at[1], hy_rs.at[par, 1], (r, g - 1))
        pl.when(r < n_res - 1)(x_up.start)
        pl.when(r > 0)(x_dn.start)
        pl.when(g < n_grp - 1)(y_up.start)
        pl.when(g > 0)(y_dn.start)

        @pl.when(odd)
        def _():
            @pl.when(j > 1)
            def _():
                om, al = wide(kept(OMEGA)), wide(kept(ALPHA))
                for i, x in tiles:
                    q = fld[Q, i, x]
                    fld[X, i, x] = fld[X, i, x] + al * fld[PP, i, x] + om * q
                    fld[R, i, x] = q - om * fld[Y, i, x]

            totals = [jnp.zeros((8, 128), F32)] * 4
            for i, x in tiles:
                shadow = fld[R0, i, x]
                for k, field in enumerate((R, W, S, Z)):
                    totals[k] = totals[k] + fold(shadow * fld[field, i, x])
            sums_start(totals, par)

        pl.when(jnp.logical_not(odd) & (j > 0))(lambda: odd_rest(par))

        @pl.when(first)
        def _():
            for copy in face_loads:
                copy.wait()
            for x in range(2):
                for i in range(3):
                    for k in range(3):
                        total = diag[i, k, x]
                        for f in range(6):
                            total = total + trans[f, i, k, x]
                        diag[i, k, x] = total
            for copy in inverse_loads:
                copy.wait()

        for x in range(2):
            for yt in range(2):
                ys = slice(yt * 8, yt * 8 + 8)
                sums = [None] * 3
                for k in range(3):
                    v = fld[src, k, x, ys, :]
                    zp = jnp.where(lane512 == 511, 0.0, pltpu.roll(v, 511, 1))
                    zm = jnp.where(lane512 == 0, 0.0, pltpu.roll(v, 1, 1))
                    if yt == 0:
                        yp = fld[src, k, x, 1:9, :]
                        ym = jnp.where(row8 == 0, 0.0, pltpu.roll(v, 1, 0))
                    else:
                        yp = jnp.where(row8 == 7, 0.0, pltpu.roll(v, 7, 0))
                        ym = fld[src, k, x, 7:15, :]
                    xn = fld[src, k, 1 - x, ys, :]
                    for i in range(3):
                        part = diag[i, k, x, ys, :] * v
                        part = part - trans[x, i, k, x, ys, :] * xn
                        part = part - trans[2, i, k, x, ys, :] * yp
                        part = part - trans[3, i, k, x, ys, :] * ym
                        part = part - trans[4, i, k, x, ys, :] * zp
                        part = part - trans[5, i, k, x, ys, :] * zm
                        sums[i] = part if sums[i] is None else sums[i] + part
                for i in range(3):
                    fld[dst, i, x, ys, :] = sums[i]

        lane128 = lax.broadcasted_iota(jnp.int32, (256, 128), 1)
        v_copies = {}
        for d in (0, 1, 3, 2):
            home = (g + d) & (n_grp - 1)
            if d == 0:
                c4 = csend[0]
            else:
                remote(csend.at[d], crecv.at[par, d], c_ss.at[d], c_rs.at[par, d], (r, home)).wait_recv()
                c4 = crecv[par, d]
            columns = jnp.zeros((256, 128), F32)
            for k in range(4):
                column = jnp.sum(inv[home, k] * c4[k : k + 1, :], axis=1, keepdims=True)
                columns = jnp.where(lane128 == k, column, columns)
            values = jnp.transpose(columns)[0:4]
            if d == 0:
                vrecv[par, 0] = values
            else:
                vsend[d] = values
                v_copies[d] = remote(
                    vsend.at[d], vrecv.at[par, 4 - d], v_ss.at[d], v_rs.at[par, 4 - d], (r, home)
                )
                v_copies[d].start()

        pl.when(r > 0)(x_up.wait_recv)
        pl.when(r < n_res - 1)(x_dn.wait_recv)
        pl.when(g > 0)(y_up.wait_recv)
        pl.when(g < n_grp - 1)(y_dn.wait_recv)
        for x in range(2):
            side, face = (0, 1) if x == 0 else (1, 0)
            for i in range(3):
                part = trans[face, i, 0, x] * hx[par, side, 0]
                for k in range(1, 3):
                    part = part + trans[face, i, k, x] * hx[par, side, k]
                low_y = trans[3, i, 0, x, 0:8, :] * hy[par, 0, x : x + 1, :]
                high_y = trans[2, i, 0, x, 8:16, :] * hy[par, 1, x : x + 1, :]
                for k in range(1, 3):
                    at = slice(k * 2 + x, k * 2 + x + 1)
                    low_y = low_y + trans[3, i, k, x, 0:8, :] * hy[par, 0, at, :]
                    high_y = high_y + trans[2, i, k, x, 8:16, :] * hy[par, 1, at, :]
                low = fld[dst, i, x, 0:8, :] - part[0:8]
                fld[dst, i, x, 0:8, :] = low - jnp.where(row8 == 0, low_y, 0.0)
                high = fld[dst, i, x, 8:16, :] - part[8:16]
                fld[dst, i, x, 8:16, :] = high - jnp.where(row8 == 7, high_y, 0.0)

        pl.when(r < n_res - 1)(x_up.wait_send)
        pl.when(r > 0)(x_dn.wait_send)
        pl.when(g < n_grp - 1)(y_up.wait_send)
        pl.when(g > 0)(y_dn.wait_send)
        for d in (1, 2, 3):
            c_copies[d].wait_send()
            v_copies[d].wait_send()

        pl.when(j > 0)(lambda: sums_wait(par))
        for d in (1, 3, 2):
            remote(vsend.at[d], vrecv.at[par, d], v_ss.at[d], v_rs.at[par, d], (r, g)).wait_recv()

        back = [vrecv[par, d] for d in range(4)]
        for b in range(8):
            part = jnp.zeros((4, 256), F32)
            for d in range(4):
                part = jnp.where(iota4 == target[b] - 4 * d, back[d], part)
            value = jnp.sum(part, axis=0, keepdims=True)
            for i in range(3):
                term = jnp.broadcast_to(w2c[i, b : b + 1, :] * value, (32, 256))
                top = term.astype(BF16)
                rest = (term - top.astype(F32)).astype(BF16)
                for zh in range(2):
                    at = zh * 96 + i * 32
                    xs[at : at + 32, b * 256 : (b + 1) * 256] = hot[b, zh] * top
                    xs[192 + at : 192 + at + 32, b * 256 : (b + 1) * 256] = hot[b, zh] * rest
        got = jnp.dot(xs[...], spread[...], preferred_element_type=F32)
        got = got[:192] + got[192:]

        d0, d1, d2, d3 = sums_of(par)
        rho, alpha, omega = kept(RHO), kept(ALPHA), kept(OMEGA)
        beta = jnp.where(j == 1, 0.0, d0 / rho * (alpha / omega))
        alpha_next = d0 / (d1 + beta * (d2 - omega * d3))
        omega_next = d0 / d1
        even = jnp.logical_not(odd) & (j > 0)
        keep(RHO, jnp.where(odd, d0, rho))
        keep(ALPHA, jnp.where(odd, alpha_next, alpha))
        keep(BETA, beta)
        keep(OMEGA, jnp.where(even, omega_next, omega))

        outer = wide(jnp.where(odd, beta, -omega_next))
        inner = wide(jnp.where(odd, omega, alpha))
        for zh in range(2):
            for i in range(3):
                for x in range(2):
                    at = zh * 96 + i * 32 + x * 16
                    zs = slice(zh * 256, (zh + 1) * 256)
                    fld[dst, i, x, :, zs] = fld[dst, i, x, :, zs] - got[at : at + 16]

        @pl.when(j > 0)
        def _():
            base = jnp.where(odd, T, Y)
            last = jnp.where(odd, Z, T)
            new = jnp.where(odd, Z, W)
            kept_in = jnp.where(odd, Q, SPARE)
            for i, x in tiles:
                old = fld[last, i, x]
                value = fld[base, i, x] + outer * (old - inner * fld[V, i, x])

                fld[kept_in, i, x] = old
                fld[new, i, x] = value

        return carry

    lax.fori_loop(0, 2 * ITERS, step, 0)
    odd_rest(0)
    sums_wait(0)
    inner, square, _, _ = sums_of(0)
    om, al = wide(inner / square), wide(kept(ALPHA))
    for i, x in tiles:
        q = fld[Q, i, x]
        fld[X, i, x] = fld[X, i, x] + al * fld[PP, i, x] + om * q
        fld[R, i, x] = q - om * fld[Y, i, x]
    outs = [
        pltpu.make_async_copy(fld.at[X], x_out, out_sem.at[0]),
        pltpu.make_async_copy(fld.at[R], r_out, out_sem.at[1]),
    ]
    for copy in outs:
        copy.start()
    for copy in outs:
        copy.wait()


def solution(mesh):
    n_res, n_grp = mesh.shape["res"], mesh.shape["grp"]
    n_dev = n_res * n_grp

    def body(right_side, accumulation, transmissibility, completion, live_count, owner, c2w, w2c, inverse):
        dma = pltpu.SemaphoreType.DMA
        field = (3, 2, 16, 512)
        any_space = pl.BlockSpec(memory_space=pl.ANY)
        return pl.pallas_call(
            functools.partial(kernel, n_res, n_grp),
            name="bicgstab",
            out_shape=[jax.ShapeDtypeStruct(field, F32)] * 2,
            in_specs=[any_space] * 9,
            out_specs=[any_space] * 2,
            scratch_shapes=[
                pltpu.SMEM((8,), jnp.int32),
                pltpu.SMEM((1, 8), jnp.int32),
                pltpu.VMEM((12,) + field, F32),
                pltpu.VMEM((3, 3, 2, 16, 512), F32),
                pltpu.VMEM((6, 3, 3, 2, 16, 512), F32),
                pltpu.VMEM((4, 4, 256, 256), F32),
                pltpu.VMEM((8, 256), jnp.int32),
                pltpu.VMEM((3, 8, 256), F32),
                pltpu.VMEM((3, 8, 256), F32),
                pltpu.VMEM((8, 256, 256), BF16),
                pltpu.VMEM((2048, 256), BF16),
                pltpu.VMEM((8, 2, 32, 256), BF16),
                pltpu.VMEM((8, 192, 256), F32),
                pltpu.VMEM((384, 256), BF16),
                pltpu.VMEM((384, 2048), BF16),
                pltpu.VMEM((2, 2, 3, 16, 512), F32),
                pltpu.VMEM((2, 2, 8, 512), F32),
                pltpu.VMEM((2, 8, 512), F32),
                pltpu.VMEM((4, 4, 256), F32),
                pltpu.VMEM((2, 4, 4, 256), F32),
                pltpu.VMEM((4, 4, 256), F32),
                pltpu.VMEM((2, 4, 4, 256), F32),
                pltpu.VMEM((1, 1, 128), F32),
                pltpu.VMEM((2, n_dev, 1, 128), F32),
                pltpu.VMEM((4, 8, 128), F32),
                dma((18,)),
                dma((2,)),
                dma((2, 2)),
                dma((2,)),
                dma((2, 2)),
                dma((4,)),
                dma((2, 4)),
                dma((4,)),
                dma((2, 4)),
                dma(()),
                dma((2,)),
                dma((2,)),
            ],
            compiler_params=pltpu.CompilerParams(collective_id=0, has_side_effects=True),
        )(
            live_count,
            owner.T,
            right_side,
            accumulation,
            transmissibility,
            completion,
            jnp.transpose(c2w, (1, 0, 2)),
            jnp.transpose(w2c, (1, 0, 2)),
            inverse,
        )

    in_specs = (
        P(None, "res", "grp", None),
        P(None, None, "res", "grp", None),
        P(None, None, None, "res", "grp", None),
        P(RES_GRP, None),
        P(RES_GRP),
        P(RES_GRP, None),
        P(RES_GRP, None, None),
        P(RES_GRP, None, None),
        P(RES_GRP, None, None, None, None),
    )
    out_specs = (P(None, "res", "grp", None), P(None, "res", "grp", None))

    def run(*args):
        first, second = jax.shard_map(
            body, mesh=mesh, in_specs=in_specs, out_specs=out_specs, check_vma=False
        )(*args)
        return first, second

    return run
```

```python
import functools

import jax
import jax.numpy as jnp
from jax import lax
from jax.experimental import pallas as pl
from jax.experimental.pallas import tpu as pltpu
from jax.sharding import PartitionSpec as P

ITERS = 3
TOGETHER = 8
RES_GRP = ("res", "grp")
MESH, LOGICAL = pl.DeviceIdType.MESH, pl.DeviceIdType.LOGICAL
F32, BF16 = jnp.float32, jnp.bfloat16
R0, R, W, T, PP, S, Z, V, X, Q, Y = range(11)


def kernel(
    n_res,
    n_grp,
    live_hbm,
    owner_hbm,
    rhs_hbm,
    acc_hbm,
    trans_hbm,
    comp_hbm,
    c2w_hbm,
    w2c_hbm,
    inv_hbm,
    x_out,
    r_out,
    live,
    owner,
    fld,
    diag,
    trans,
    inv,
    comp,
    c2w,
    w2c,
    picks,
    spread,
    hot,
    grid_of,
    lhs,
    xs,
    hx,
    hy,
    ysend,
    csend,
    crecv,
    vsend,
    vrecv,
    rsend,
    rrecv,
    scal,
    in_sem,
    hx_ss,
    hx_rs,
    hy_ss,
    hy_rs,
    c_ss,
    c_rs,
    v_ss,
    v_rs,
    r_ss,
    r_rs,
):
    n_dev = n_res * n_grp
    r, g = lax.axis_index("res"), lax.axis_index("grp")
    me = r * n_grp + g

    def load(i, src, dst):
        return pltpu.make_async_copy(src, dst, in_sem.at[i])

    first_loads = [
        load(0, comp_hbm, comp),
        load(1, live_hbm, live),
        load(2, owner_hbm, owner),
        load(3, c2w_hbm, c2w),
        load(4, w2c_hbm, w2c),
        load(5, rhs_hbm, fld.at[R0]),
        load(6, rhs_hbm, fld.at[R]),
    ]
    face_loads = [load(7, acc_hbm, diag)] + [load(8 + f, trans_hbm.at[f], trans.at[f]) for f in range(6)]
    inverse_loads = [load(14 + h, inv_hbm.at[0, h], inv.at[h]) for h in range(4)]
    for copy in first_loads + face_loads + inverse_loads:
        copy.start()

    hx[...] = jnp.zeros_like(hx)
    hy[...] = jnp.zeros_like(hy)
    rrecv[...] = jnp.zeros_like(rrecv)

    barrier = pltpu.get_barrier_semaphore()

    def peer(k):
        return (me + k) & (n_dev - 1)

    def every_peer(act):
        trips, last = divmod(n_dev - 1, TOGETHER)

        def trip(m, carry):
            for u in range(TOGETHER):
                act(1 + m * TOGETHER + u)
            return carry

        lax.fori_loop(0, trips, trip, 0)
        for u in range(last):
            act(1 + trips * TOGETHER + u)

    every_peer(lambda k: pl.semaphore_signal(barrier, inc=1, device_id=peer(k), device_id_type=LOGICAL))

    for field in (W, T, PP, S, Z, V, X, Q, Y):
        fld[field] = jnp.zeros((3, 2, 16, 512), F32)
    scal[...] = jnp.zeros_like(scal)
    csend[...] = jnp.zeros_like(csend)
    ysend[...] = jnp.zeros_like(ysend)

    for copy in first_loads[:5]:
        copy.wait()
    owners = [owner[0, b] for b in range(8)]
    target = []
    for b in range(8):
        slot = jnp.int32(0)
        for a in range(b):
            slot = slot + jnp.where(owners[a] == owners[b], 1, 0).astype(jnp.int32)
        target.append(((owners[b] - g) & (n_grp - 1)) * 4 + slot)

    seg = lax.broadcasted_iota(jnp.int32, (8, 256), 1)
    well = lax.broadcasted_iota(jnp.int32, (8, 256), 0)
    lives = jnp.zeros((8, 256), jnp.int32)
    for b in range(8):
        lives = jnp.where(well == b, live[b], lives)
    for i in range(3):
        c2w[i] = jnp.where(seg < lives, c2w[i], 0.0)
        w2c[i] = jnp.where(seg < lives, w2c[i], 0.0)
    for b in range(8):
        cell = comp[b : b + 1, :]
        low = cell & 255
        half = (cell >> 8) & 1
        high = cell >> 9
        one = jnp.where(lax.broadcasted_iota(jnp.int32, (256, 256), 0) == low, 1.0, 0.0).astype(F32)
        picks[b] = one.astype(BF16)
        spread[b * 256 : (b + 1) * 256, :] = jnp.transpose(one).astype(BF16)
        rows = lax.broadcasted_iota(jnp.int32, (32, 256), 0)
        for zh in range(2):
            here = (rows == high) & (half == zh)
            hot[b, zh] = jnp.where(here, 1.0, 0.0).astype(BF16)
            for i in range(3):
                grid_of[b, zh * 96 + i * 32 : zh * 96 + (i + 1) * 32, :] = jnp.where(
                    here, c2w[i, b : b + 1, :], 0.0
                )
    for copy in first_loads[5:]:
        copy.wait()

    def remote(src, dst, ss, rs, device):
        return pltpu.make_async_remote_copy(
            src_ref=src, dst_ref=dst, send_sem=ss, recv_sem=rs, device_id=device, device_id_type=MESH
        )

    lane512 = lax.broadcasted_iota(jnp.int32, (8, 512), 1)
    row8 = lax.broadcasted_iota(jnp.int32, (8, 512), 0)
    iota4 = lax.broadcasted_iota(jnp.int32, (4, 256), 0)
    iota16 = lax.broadcasted_iota(jnp.int32, (16, 256), 0)
    lane = lax.broadcasted_iota(jnp.int32, (1, 128), 1)
    RHO, ALPHA, OMEGA, BETA = 0, 1, 2, 3

    def keep(at, value):
        scal[at] = jnp.broadcast_to(value, (8, 128))

    def kept(at):
        return scal[at, 0:1, 0:1]

    def wide(value):
        return jnp.broadcast_to(value, (16, 512))

    def fold(block):
        half = block[0:8] + block[8:16]
        return (half[:, 0:128] + half[:, 128:256]) + (half[:, 256:384] + half[:, 384:512])

    def row_of(totals):
        row = jnp.zeros((1, 128), F32)
        for k, total in enumerate(totals):
            one = jnp.sum(jnp.sum(total, axis=0, keepdims=True), axis=1, keepdims=True)
            row = jnp.where(lane == k, one, row)
        return row

    def sums_start(row, par):
        rsend[0] = row
        rrecv[par, me] = row

        def send(k):
            pltpu.make_async_remote_copy(
                src_ref=rsend,
                dst_ref=rrecv.at[par, pl.ds(me, 1)],
                send_sem=r_ss,
                recv_sem=r_rs.at[par],
                device_id=peer(k),
                device_id_type=LOGICAL,
            ).start()

        every_peer(send)

    def sums_wait(par):
        some = rrecv.at[par, pl.ds(0, n_dev - 1)]
        pltpu.make_async_copy(some, some, r_rs.at[par]).wait()
        pltpu.make_async_copy(some, some, r_ss).wait()

    def sums_of(par):
        row = jnp.sum(rrecv[par], axis=0)
        return [jnp.sum(jnp.where(lane == k, row, 0.0), axis=1, keepdims=True) for k in range(4)]

    tiles = [(i, x) for i in range(3) for x in range(2)]

    def odd_rest():
        be, om, al = wide(kept(BETA)), wide(kept(OMEGA)), wide(kept(ALPHA))
        inner, square = jnp.zeros((8, 128), F32), jnp.zeros((8, 128), F32)
        for i, x in tiles:
            s, res, w = fld[S, i, x], fld[R, i, x], fld[W, i, x]
            fld[PP, i, x] = res + be * (fld[PP, i, x] - om * s)
            s = w + be * (s - om * fld[Q, i, x])
            fld[S, i, x] = s
            q = res - al * s
            y = w - al * fld[Z, i, x]
            fld[Q, i, x] = q
            fld[Y, i, x] = y
            inner = inner + fold(q * y)
            square = square + fold(y * y)
        return row_of([inner, square])

    def phase(it, odd):
        par = int(odd)
        first = it == 0
        src = W if odd else jnp.where(first, R, Z)
        dst = T if odd else jnp.where(first, W, V)

        if odd:
            om, al = wide(kept(OMEGA)), wide(kept(ALPHA))
            totals = [jnp.zeros((8, 128), F32)] * 4
            for i, x in tiles:
                q = fld[Q, i, x]
                fld[X, i, x] = fld[X, i, x] + al * fld[PP, i, x] + om * q
                res = q - om * fld[Y, i, x]
                fld[R, i, x] = res
                shadow = fld[R0, i, x]
                for k, value in enumerate((res, fld[W, i, x], fld[S, i, x], fld[Z, i, x])):
                    totals[k] = totals[k] + fold(shadow * value)
            parts = row_of(totals)
        else:
            parts = odd_rest()

        for zh in range(2):
            v = fld[src, :, :, :, zh * 256 : (zh + 1) * 256].reshape(96, 256)
            top = v.astype(BF16)
            lhs[zh * 96 : (zh + 1) * 96, :] = top
            lhs[192 + zh * 96 : 192 + (zh + 1) * 96, :] = (v - top.astype(F32)).astype(BF16)
        out = jnp.zeros((16, 256), F32)
        for b in range(8):
            got = jnp.dot(lhs[...], picks[b], preferred_element_type=F32)
            row = jnp.sum((got[:192] + got[192:]) * grid_of[b], axis=0, keepdims=True)
            out = jnp.where(iota16 == target[b], row, out)
        for d in range(4):
            csend[d] = out[d * 4 : (d + 1) * 4]
        for k in range(2):
            for x in range(2):
                for j3 in range(3):
                    at = j3 * 2 + x
                    edge = 15 if k == 0 else 0
                    ysend[k, at : at + 1, :] = fld[src, j3, x, edge : edge + 1, :]

        if not odd:

            @pl.when(first)
            def _():
                pl.semaphore_wait(barrier, n_dev - 1)

        c_copies = {}
        for d in (2, 1, 3):
            to = (r, (g + d) & (n_grp - 1))
            c_copies[d] = remote(csend.at[d], crecv.at[par, 4 - d], c_ss.at[d], c_rs.at[par, 4 - d], to)
            c_copies[d].start()

        x_up = remote(fld.at[src, :, 1], hx.at[par, 0], hx_ss.at[0], hx_rs.at[par, 0], (r + 1, g))
        x_dn = remote(fld.at[src, :, 0], hx.at[par, 1], hx_ss.at[1], hx_rs.at[par, 1], (r - 1, g))
        y_up = remote(ysend.at[0], hy.at[par, 0], hy_ss.at[0], hy_rs.at[par, 0], (r, g + 1))
        y_dn = remote(ysend.at[1], hy.at[par, 1], hy_ss.at[1], hy_rs.at[par, 1], (r, g - 1))
        pl.when(r < n_res - 1)(x_up.start)
        pl.when(r > 0)(x_dn.start)
        pl.when(g < n_grp - 1)(y_up.start)
        pl.when(g > 0)(y_dn.start)
        if odd:
            sums_start(parts, par)
        else:
            pl.when(it > 0)(lambda: sums_start(parts, par))

        if not odd:

            @pl.when(first)
            def _():
                for copy in face_loads:
                    copy.wait()
                for x in range(2):
                    for i in range(3):
                        for k in range(3):
                            total = diag[i, k, x]
                            for f in range(6):
                                total = total + trans[f, i, k, x]
                            diag[i, k, x] = total
                for copy in inverse_loads:
                    copy.wait()

        for x in range(2):
            for yt in range(2):
                ys = slice(yt * 8, yt * 8 + 8)
                sums = [None] * 3
                for k in range(3):
                    v = fld[src, k, x, ys, :]
                    zp = jnp.where(lane512 == 511, 0.0, pltpu.roll(v, 511, 1))
                    zm = jnp.where(lane512 == 0, 0.0, pltpu.roll(v, 1, 1))
                    if yt == 0:
                        yp = fld[src, k, x, 1:9, :]
                        ym = jnp.where(row8 == 0, 0.0, pltpu.roll(v, 1, 0))
                    else:
                        yp = jnp.where(row8 == 7, 0.0, pltpu.roll(v, 7, 0))
                        ym = fld[src, k, x, 7:15, :]
                    xn = fld[src, k, 1 - x, ys, :]
                    for i in range(3):
                        part = diag[i, k, x, ys, :] * v
                        part = part - trans[x, i, k, x, ys, :] * xn
                        part = part - trans[2, i, k, x, ys, :] * yp
                        part = part - trans[3, i, k, x, ys, :] * ym
                        part = part - trans[4, i, k, x, ys, :] * zp
                        part = part - trans[5, i, k, x, ys, :] * zm
                        sums[i] = part if sums[i] is None else sums[i] + part
                for i in range(3):
                    fld[dst, i, x, ys, :] = sums[i]

        lane128 = lax.broadcasted_iota(jnp.int32, (256, 128), 1)
        v_copies = {}
        for d in (0, 1, 3, 2):
            home = (g + d) & (n_grp - 1)
            if d == 0:
                c4 = csend[0]
            else:
                remote(csend.at[d], crecv.at[par, d], c_ss.at[d], c_rs.at[par, d], (r, home)).wait_recv()
                c4 = crecv[par, d]
            columns = jnp.zeros((256, 128), F32)
            for k in range(4):
                column = jnp.sum(inv[home, k] * c4[k : k + 1, :], axis=1, keepdims=True)
                columns = jnp.where(lane128 == k, column, columns)
            values = jnp.transpose(columns)[0:4]
            if d == 0:
                vrecv[par, 0] = values
            else:
                vsend[d] = values
                v_copies[d] = remote(
                    vsend.at[d], vrecv.at[par, 4 - d], v_ss.at[d], v_rs.at[par, 4 - d], (r, home)
                )
                v_copies[d].start()

        pl.when(r > 0)(x_up.wait_recv)
        pl.when(r < n_res - 1)(x_dn.wait_recv)
        pl.when(g > 0)(y_up.wait_recv)
        pl.when(g < n_grp - 1)(y_dn.wait_recv)
        for x in range(2):
            side, face = (0, 1) if x == 0 else (1, 0)
            for i in range(3):
                part = trans[face, i, 0, x] * hx[par, side, 0]
                for k in range(1, 3):
                    part = part + trans[face, i, k, x] * hx[par, side, k]
                low_y = trans[3, i, 0, x, 0:8, :] * hy[par, 0, x : x + 1, :]
                high_y = trans[2, i, 0, x, 8:16, :] * hy[par, 1, x : x + 1, :]
                for k in range(1, 3):
                    at = slice(k * 2 + x, k * 2 + x + 1)
                    low_y = low_y + trans[3, i, k, x, 0:8, :] * hy[par, 0, at, :]
                    high_y = high_y + trans[2, i, k, x, 8:16, :] * hy[par, 1, at, :]
                low = fld[dst, i, x, 0:8, :] - part[0:8]
                fld[dst, i, x, 0:8, :] = low - jnp.where(row8 == 0, low_y, 0.0)
                high = fld[dst, i, x, 8:16, :] - part[8:16]
                fld[dst, i, x, 8:16, :] = high - jnp.where(row8 == 7, high_y, 0.0)

        pl.when(r < n_res - 1)(x_up.wait_send)
        pl.when(r > 0)(x_dn.wait_send)
        pl.when(g < n_grp - 1)(y_up.wait_send)
        pl.when(g > 0)(y_dn.wait_send)
        for d in (1, 2, 3):
            c_copies[d].wait_send()
            v_copies[d].wait_send()

        if odd:
            sums_wait(par)
        else:
            pl.when(it > 0)(lambda: sums_wait(par))
        d0, d1, d2, d3 = sums_of(par)
        rho, alpha, omega = kept(RHO), kept(ALPHA), kept(OMEGA)
        if odd:
            beta = jnp.where(first, 0.0, d0 / rho * (alpha / omega))
            alpha_next = d0 / (d1 + beta * (d2 - omega * d3))
            keep(RHO, d0)
            keep(ALPHA, alpha_next)
            keep(BETA, beta)
            outer, inner = wide(beta), wide(omega)
        else:
            omega_next = jnp.where(first, 0.0, d0 / d1)
            keep(OMEGA, omega_next)
            outer, inner = wide(-omega_next), wide(alpha)

        for d in (1, 3, 2):
            remote(vsend.at[d], vrecv.at[par, d], v_ss.at[d], v_rs.at[par, d], (r, g)).wait_recv()

        back = [vrecv[par, d] for d in range(4)]
        for b in range(8):
            part = jnp.zeros((4, 256), F32)
            for d in range(4):
                part = jnp.where(iota4 == target[b] - 4 * d, back[d], part)
            value = jnp.sum(part, axis=0, keepdims=True)
            for i in range(3):
                term = jnp.broadcast_to(w2c[i, b : b + 1, :] * value, (32, 256))
                top = term.astype(BF16)
                rest = (term - top.astype(F32)).astype(BF16)
                for zh in range(2):
                    at = zh * 96 + i * 32
                    xs[at : at + 32, b * 256 : (b + 1) * 256] = hot[b, zh] * top
                    xs[192 + at : 192 + at + 32, b * 256 : (b + 1) * 256] = hot[b, zh] * rest
        got = jnp.dot(xs[...], spread[...], preferred_element_type=F32)
        got = got[:192] + got[192:]

        for zh in range(2):
            for i in range(3):
                for x in range(2):
                    at = zh * 96 + i * 32 + x * 16
                    zs = slice(zh * 256, (zh + 1) * 256)
                    fld[dst, i, x, :, zs] = fld[dst, i, x, :, zs] - got[at : at + 16]

        if odd:
            for i, x in tiles:
                old = fld[Z, i, x]
                fld[Q, i, x] = old
                fld[Z, i, x] = fld[T, i, x] + outer * (old - inner * fld[V, i, x])
        else:

            @pl.when(it > 0)
            def _():
                for i, x in tiles:
                    fld[W, i, x] = fld[Y, i, x] + outer * (fld[T, i, x] - inner * fld[V, i, x])

    def step(it, carry):
        phase(it, False)
        phase(it, True)
        return carry

    lax.fori_loop(0, ITERS, step, 0)
    sums_start(odd_rest(), 0)
    sums_wait(0)
    inner, square, _, _ = sums_of(0)
    om, al = wide(inner / square), wide(kept(ALPHA))
    for i, x in tiles:
        q = fld[Q, i, x]
        x_out[i, x] = fld[X, i, x] + al * fld[PP, i, x] + om * q
        r_out[i, x] = q - om * fld[Y, i, x]


def hand_out(x_in, r_in, x_out, r_out, sem):
    outs = [pltpu.make_async_copy(x_in, x_out, sem.at[0]), pltpu.make_async_copy(r_in, r_out, sem.at[1])]
    for copy in outs:
        copy.start()
    for copy in outs:
        copy.wait()


def solution(mesh):
    n_res, n_grp = mesh.shape["res"], mesh.shape["grp"]
    n_dev = n_res * n_grp

    def body(right_side, accumulation, transmissibility, completion, live_count, owner, c2w, w2c, inverse):
        dma = pltpu.SemaphoreType.DMA
        field = (3, 2, 16, 512)
        any_space = pl.BlockSpec(memory_space=pl.ANY)
        vmem = pl.BlockSpec(memory_space=pltpu.VMEM)
        operands = (
            live_count,
            owner.T,
            right_side,
            accumulation,
            transmissibility,
            completion,
            jnp.transpose(c2w, (1, 0, 2)),
            jnp.transpose(w2c, (1, 0, 2)),
            inverse,
        )
        operands = [pltpu.with_memory_space_constraint(a, pltpu.HBM) for a in operands]
        held = pl.pallas_call(
            functools.partial(kernel, n_res, n_grp),
            name="bicgstab",
            out_shape=[jax.ShapeDtypeStruct(field, F32)] * 2,
            in_specs=[any_space] * 9,
            out_specs=[vmem] * 2,
            scratch_shapes=[
                pltpu.SMEM((8,), jnp.int32),
                pltpu.SMEM((1, 8), jnp.int32),
                pltpu.VMEM((11,) + field, F32),
                pltpu.VMEM((3, 3, 2, 16, 512), F32),
                pltpu.VMEM((6, 3, 3, 2, 16, 512), F32),
                pltpu.VMEM((4, 4, 256, 256), F32),
                pltpu.VMEM((8, 256), jnp.int32),
                pltpu.VMEM((3, 8, 256), F32),
                pltpu.VMEM((3, 8, 256), F32),
                pltpu.VMEM((8, 256, 256), BF16),
                pltpu.VMEM((2048, 256), BF16),
                pltpu.VMEM((8, 2, 32, 256), BF16),
                pltpu.VMEM((8, 192, 256), F32),
                pltpu.VMEM((384, 256), BF16),
                pltpu.VMEM((384, 2048), BF16),
                pltpu.VMEM((2, 2, 3, 16, 512), F32),
                pltpu.VMEM((2, 2, 8, 512), F32),
                pltpu.VMEM((2, 8, 512), F32),
                pltpu.VMEM((4, 4, 256), F32),
                pltpu.VMEM((2, 4, 4, 256), F32),
                pltpu.VMEM((4, 4, 256), F32),
                pltpu.VMEM((2, 4, 4, 256), F32),
                pltpu.VMEM((1, 1, 128), F32),
                pltpu.VMEM((2, n_dev, 1, 128), F32),
                pltpu.VMEM((4, 8, 128), F32),
                dma((18,)),
                dma((2,)),
                dma((2, 2)),
                dma((2,)),
                dma((2, 2)),
                dma((4,)),
                dma((2, 4)),
                dma((4,)),
                dma((2, 4)),
                dma(()),
                dma((2,)),
            ],
            compiler_params=pltpu.CompilerParams(
                collective_id=0, has_side_effects=True, vmem_limit_bytes=24 << 20
            ),
        )(*operands)
        return pl.pallas_call(
            hand_out,
            name="hand_out",
            out_shape=[jax.ShapeDtypeStruct(field, F32)] * 2,
            in_specs=[vmem] * 2,
            out_specs=[any_space] * 2,
            scratch_shapes=[dma((2,))],
            compiler_params=pltpu.CompilerParams(vmem_limit_bytes=1 << 20),
        )(*held)

    in_specs = (
        P(None, "res", "grp", None),
        P(None, None, "res", "grp", None),
        P(None, None, None, "res", "grp", None),
        P(RES_GRP, None),
        P(RES_GRP),
        P(RES_GRP, None),
        P(RES_GRP, None, None),
        P(RES_GRP, None, None),
        P(RES_GRP, None, None, None, None),
    )
    out_specs = (P(None, "res", "grp", None), P(None, "res", "grp", None))

    def run(*args):
        first, second = jax.shard_map(
            body, mesh=mesh, in_specs=in_specs, out_specs=out_specs, check_vma=False
        )(*args)
        return first, second

    return run
```

```python
import functools

import jax
import jax.numpy as jnp
from jax import lax
from jax.experimental import pallas as pl
from jax.experimental.pallas import tpu as pltpu
from jax.sharding import PartitionSpec as P

ITERS = 3
TOGETHER = 8
RES_GRP = ("res", "grp")
MESH, LOGICAL = pl.DeviceIdType.MESH, pl.DeviceIdType.LOGICAL
F32, BF16 = jnp.float32, jnp.bfloat16
R0, R, W, T, PP, S, Z, V, X, Q, Y = range(11)


def kernel(
    n_res,
    n_grp,
    live_hbm,
    owner_hbm,
    rhs_hbm,
    acc_hbm,
    trans_hbm,
    comp_hbm,
    c2w_hbm,
    w2c_hbm,
    inv_hbm,
    x_out,
    r_out,
    live,
    owner,
    fld,
    diag,
    trans,
    inv,
    comp,
    c2w,
    w2c,
    picks,
    spread,
    hot,
    grid_of,
    lhs,
    xs,
    hx,
    hy,
    ysend,
    csend,
    crecv,
    vsend,
    vrecv,
    pair,
    rsend,
    rrecv,
    scal,
    in_sem,
    hx_ss,
    hx_rs,
    hy_ss,
    hy_rs,
    c_ss,
    c_rs,
    v_ss,
    v_rs,
    p_ss,
    p_rs,
    r_ss,
    r_rs,
):
    n_dev = n_res * n_grp
    r, g = lax.axis_index("res"), lax.axis_index("grp")

    def load(i, src, dst):
        return pltpu.make_async_copy(src, dst, in_sem.at[i])

    first_loads = [
        load(0, comp_hbm, comp),
        load(1, live_hbm, live),
        load(2, owner_hbm, owner),
        load(3, c2w_hbm, c2w),
        load(4, w2c_hbm, w2c),
        load(5, rhs_hbm, fld.at[R0]),
        load(6, rhs_hbm, fld.at[R]),
    ]
    face_loads = [load(7, acc_hbm, diag)] + [load(8 + f, trans_hbm.at[f], trans.at[f]) for f in range(6)]
    inverse_loads = [load(14 + h, inv_hbm.at[0, h], inv.at[h]) for h in range(4)]
    for copy in first_loads + face_loads + inverse_loads:
        copy.start()

    hx[...] = jnp.zeros_like(hx)
    hy[...] = jnp.zeros_like(hy)
    rrecv[...] = jnp.zeros_like(rrecv)

    barrier = pltpu.get_barrier_semaphore()

    chips = n_dev // 2
    core = r & 1
    chip = (r >> 1) * n_grp + g
    mate = (r + 1 - 2 * core, g)
    beside = r - 1 + 2 * core
    has_beside = (beside >= 0) & (beside < n_res)

    def teammate(k):
        other = (chip + k) & (chips - 1)
        return ((other >> (n_grp.bit_length() - 1)) * 2 + core) * n_grp + (other & (n_grp - 1))

    def every_teammate(act):
        trips, last = divmod(chips - 1, TOGETHER)

        def trip(m, carry):
            for u in range(TOGETHER):
                act(1 + m * TOGETHER + u)
            return carry

        lax.fori_loop(0, trips, trip, 0)
        for u in range(last):
            act(1 + trips * TOGETHER + u)

    every_teammate(
        lambda k: pl.semaphore_signal(barrier, inc=1, device_id=teammate(k), device_id_type=LOGICAL)
    )
    pl.semaphore_signal(barrier, inc=1, device_id=mate, device_id_type=MESH)

    @pl.when(has_beside)
    def _():
        pl.semaphore_signal(barrier, inc=1, device_id=(beside, g), device_id_type=MESH)

    for field in (W, T, PP, S, Z, V, X, Q, Y):
        fld[field] = jnp.zeros((3, 2, 16, 512), F32)
    scal[...] = jnp.zeros_like(scal)
    csend[...] = jnp.zeros_like(csend)
    ysend[...] = jnp.zeros_like(ysend)

    for copy in first_loads[:5]:
        copy.wait()
    owners = [owner[0, b] for b in range(8)]
    target = []
    for b in range(8):
        slot = jnp.int32(0)
        for a in range(b):
            slot = slot + jnp.where(owners[a] == owners[b], 1, 0).astype(jnp.int32)
        target.append(((owners[b] - g) & (n_grp - 1)) * 4 + slot)

    seg = lax.broadcasted_iota(jnp.int32, (8, 256), 1)
    well = lax.broadcasted_iota(jnp.int32, (8, 256), 0)
    lives = jnp.zeros((8, 256), jnp.int32)
    for b in range(8):
        lives = jnp.where(well == b, live[b], lives)
    for i in range(3):
        c2w[i] = jnp.where(seg < lives, c2w[i], 0.0)
        w2c[i] = jnp.where(seg < lives, w2c[i], 0.0)
    for b in range(8):
        cell = comp[b : b + 1, :]
        low = cell & 255
        half = (cell >> 8) & 1
        high = cell >> 9
        one = jnp.where(lax.broadcasted_iota(jnp.int32, (256, 256), 0) == low, 1.0, 0.0).astype(F32)
        picks[b] = one.astype(BF16)
        spread[b * 256 : (b + 1) * 256, :] = jnp.transpose(one).astype(BF16)
        rows = lax.broadcasted_iota(jnp.int32, (32, 256), 0)
        for zh in range(2):
            here = (rows == high) & (half == zh)
            hot[b, zh] = jnp.where(here, 1.0, 0.0).astype(BF16)
            for i in range(3):
                grid_of[b, zh * 96 + i * 32 : zh * 96 + (i + 1) * 32, :] = jnp.where(
                    here, c2w[i, b : b + 1, :], 0.0
                )
    for copy in first_loads[5:]:
        copy.wait()

    def remote(src, dst, ss, rs, device):
        return pltpu.make_async_remote_copy(
            src_ref=src, dst_ref=dst, send_sem=ss, recv_sem=rs, device_id=device, device_id_type=MESH
        )

    lane512 = lax.broadcasted_iota(jnp.int32, (8, 512), 1)
    row8 = lax.broadcasted_iota(jnp.int32, (8, 512), 0)
    iota4 = lax.broadcasted_iota(jnp.int32, (4, 256), 0)
    iota16 = lax.broadcasted_iota(jnp.int32, (16, 256), 0)
    lane = lax.broadcasted_iota(jnp.int32, (1, 128), 1)
    RHO, ALPHA, OMEGA, BETA = 0, 1, 2, 3

    def keep(at, value):
        scal[at] = jnp.broadcast_to(value, (8, 128))

    def kept(at):
        return scal[at, 0:1, 0:1]

    def wide(value):
        return jnp.broadcast_to(value, (16, 512))

    def fold(block):
        half = block[0:8] + block[8:16]
        return (half[:, 0:128] + half[:, 128:256]) + (half[:, 256:384] + half[:, 384:512])

    def row_of(totals):
        row = jnp.zeros((1, 128), F32)
        for k, total in enumerate(totals):
            one = jnp.sum(jnp.sum(total, axis=0, keepdims=True), axis=1, keepdims=True)
            row = jnp.where(lane == k, one, row)
        return row

    def to_mate(par):
        return remote(pair.at[0, par], pair.at[1, par], p_ss, p_rs.at[par], mate)

    def sums_start(row, par):
        pair[0, par, 0] = row
        to_mate(par).start()

    def sums_on(par):
        to_mate(par).wait()
        row = pair[0, par, 0] + pair[1, par, 0]
        rsend[0] = row
        rrecv[par, chip] = row

        def send(k):
            pltpu.make_async_remote_copy(
                src_ref=rsend,
                dst_ref=rrecv.at[par, pl.ds(chip, 1)],
                send_sem=r_ss,
                recv_sem=r_rs.at[par],
                device_id=teammate(k),
                device_id_type=LOGICAL,
            ).start()

        every_teammate(send)

    def sums_wait(par):
        some = rrecv.at[par, pl.ds(0, chips - 1)]
        pltpu.make_async_copy(some, some, r_rs.at[par]).wait()
        pltpu.make_async_copy(some, some, r_ss).wait()

    def sums_of(par):
        row = jnp.sum(rrecv[par], axis=0)
        return [jnp.sum(jnp.where(lane == k, row, 0.0), axis=1, keepdims=True) for k in range(4)]

    tiles = [(i, x) for i in range(3) for x in range(2)]

    def odd_rest():
        be, om, al = wide(kept(BETA)), wide(kept(OMEGA)), wide(kept(ALPHA))
        inner, square = jnp.zeros((8, 128), F32), jnp.zeros((8, 128), F32)
        for i, x in tiles:
            s, res, w = fld[S, i, x], fld[R, i, x], fld[W, i, x]
            fld[PP, i, x] = res + be * (fld[PP, i, x] - om * s)
            s = w + be * (s - om * fld[Q, i, x])
            fld[S, i, x] = s
            q = res - al * s
            y = w - al * fld[Z, i, x]
            fld[Q, i, x] = q
            fld[Y, i, x] = y
            inner = inner + fold(q * y)
            square = square + fold(y * y)
        return row_of([inner, square])

    def phase(it, odd):
        par = int(odd)
        first = it == 0
        src = W if odd else jnp.where(first, R, Z)
        dst = T if odd else jnp.where(first, W, V)

        if odd:
            om, al = wide(kept(OMEGA)), wide(kept(ALPHA))
            totals = [jnp.zeros((8, 128), F32)] * 4
            for i, x in tiles:
                q = fld[Q, i, x]
                fld[X, i, x] = fld[X, i, x] + al * fld[PP, i, x] + om * q
                res = q - om * fld[Y, i, x]
                fld[R, i, x] = res
                shadow = fld[R0, i, x]
                for k, value in enumerate((res, fld[W, i, x], fld[S, i, x], fld[Z, i, x])):
                    totals[k] = totals[k] + fold(shadow * value)
            parts = row_of(totals)
        else:
            parts = odd_rest()

        for zh in range(2):
            v = fld[src, :, :, :, zh * 256 : (zh + 1) * 256].reshape(96, 256)
            top = v.astype(BF16)
            lhs[zh * 96 : (zh + 1) * 96, :] = top
            lhs[192 + zh * 96 : 192 + (zh + 1) * 96, :] = (v - top.astype(F32)).astype(BF16)
        out = jnp.zeros((16, 256), F32)
        for b in range(8):
            got = jnp.dot(lhs[...], picks[b], preferred_element_type=F32)
            row = jnp.sum((got[:192] + got[192:]) * grid_of[b], axis=0, keepdims=True)
            out = jnp.where(iota16 == target[b], row, out)
        for d in range(4):
            csend[d] = out[d * 4 : (d + 1) * 4]
        for k in range(2):
            for x in range(2):
                for j3 in range(3):
                    at = j3 * 2 + x
                    edge = 15 if k == 0 else 0
                    ysend[k, at : at + 1, :] = fld[src, j3, x, edge : edge + 1, :]

        if not odd:

            @pl.when(first)
            def _():
                pl.semaphore_wait(barrier, chips + jnp.where(has_beside, 1, 0).astype(jnp.int32))

        c_copies = {}
        for d in (2, 1, 3):
            to = (r, (g + d) & (n_grp - 1))
            c_copies[d] = remote(csend.at[d], crecv.at[par, 4 - d], c_ss.at[d], c_rs.at[par, 4 - d], to)
            c_copies[d].start()

        x_up = remote(fld.at[src, :, 1], hx.at[par, 0], hx_ss.at[0], hx_rs.at[par, 0], (r + 1, g))
        x_dn = remote(fld.at[src, :, 0], hx.at[par, 1], hx_ss.at[1], hx_rs.at[par, 1], (r - 1, g))
        y_up = remote(ysend.at[0], hy.at[par, 0], hy_ss.at[0], hy_rs.at[par, 0], (r, g + 1))
        y_dn = remote(ysend.at[1], hy.at[par, 1], hy_ss.at[1], hy_rs.at[par, 1], (r, g - 1))
        pl.when(r < n_res - 1)(x_up.start)
        pl.when(r > 0)(x_dn.start)
        pl.when(g < n_grp - 1)(y_up.start)
        pl.when(g > 0)(y_dn.start)
        if odd:
            sums_start(parts, par)
        else:
            pl.when(it > 0)(lambda: sums_start(parts, par))

        if not odd:

            @pl.when(first)
            def _():
                for copy in face_loads:
                    copy.wait()
                for x in range(2):
                    for i in range(3):
                        for k in range(3):
                            total = diag[i, k, x]
                            for f in range(6):
                                total = total + trans[f, i, k, x]
                            diag[i, k, x] = total
                for copy in inverse_loads:
                    copy.wait()

        for x in range(2):
            for yt in range(2):
                ys = slice(yt * 8, yt * 8 + 8)
                sums = [None] * 3
                for k in range(3):
                    v = fld[src, k, x, ys, :]
                    zp = jnp.where(lane512 == 511, 0.0, pltpu.roll(v, 511, 1))
                    zm = jnp.where(lane512 == 0, 0.0, pltpu.roll(v, 1, 1))
                    if yt == 0:
                        yp = fld[src, k, x, 1:9, :]
                        ym = jnp.where(row8 == 0, 0.0, pltpu.roll(v, 1, 0))
                    else:
                        yp = jnp.where(row8 == 7, 0.0, pltpu.roll(v, 7, 0))
                        ym = fld[src, k, x, 7:15, :]
                    xn = fld[src, k, 1 - x, ys, :]
                    for i in range(3):
                        part = diag[i, k, x, ys, :] * v
                        part = part - trans[x, i, k, x, ys, :] * xn
                        part = part - trans[2, i, k, x, ys, :] * yp
                        part = part - trans[3, i, k, x, ys, :] * ym
                        part = part - trans[4, i, k, x, ys, :] * zp
                        part = part - trans[5, i, k, x, ys, :] * zm
                        sums[i] = part if sums[i] is None else sums[i] + part
                for i in range(3):
                    fld[dst, i, x, ys, :] = sums[i]

        lane128 = lax.broadcasted_iota(jnp.int32, (256, 128), 1)
        v_copies = {}
        for d in (0, 1, 3, 2):
            home = (g + d) & (n_grp - 1)
            if d == 1:
                if odd:
                    sums_on(par)
                else:
                    pl.when(it > 0)(lambda: sums_on(par))
            if d == 0:
                c4 = csend[0]
            else:
                remote(csend.at[d], crecv.at[par, d], c_ss.at[d], c_rs.at[par, d], (r, home)).wait_recv()
                c4 = crecv[par, d]
            columns = jnp.zeros((256, 128), F32)
            for k in range(4):
                column = jnp.sum(inv[home, k] * c4[k : k + 1, :], axis=1, keepdims=True)
                columns = jnp.where(lane128 == k, column, columns)
            values = jnp.transpose(columns)[0:4]
            if d == 0:
                vrecv[par, 0] = values
            else:
                vsend[d] = values
                v_copies[d] = remote(
                    vsend.at[d], vrecv.at[par, 4 - d], v_ss.at[d], v_rs.at[par, 4 - d], (r, home)
                )
                v_copies[d].start()

        pl.when(r > 0)(x_up.wait_recv)
        pl.when(r < n_res - 1)(x_dn.wait_recv)
        pl.when(g > 0)(y_up.wait_recv)
        pl.when(g < n_grp - 1)(y_dn.wait_recv)
        for x in range(2):
            side, face = (0, 1) if x == 0 else (1, 0)
            for i in range(3):
                part = trans[face, i, 0, x] * hx[par, side, 0]
                for k in range(1, 3):
                    part = part + trans[face, i, k, x] * hx[par, side, k]
                low_y = trans[3, i, 0, x, 0:8, :] * hy[par, 0, x : x + 1, :]
                high_y = trans[2, i, 0, x, 8:16, :] * hy[par, 1, x : x + 1, :]
                for k in range(1, 3):
                    at = slice(k * 2 + x, k * 2 + x + 1)
                    low_y = low_y + trans[3, i, k, x, 0:8, :] * hy[par, 0, at, :]
                    high_y = high_y + trans[2, i, k, x, 8:16, :] * hy[par, 1, at, :]
                low = fld[dst, i, x, 0:8, :] - part[0:8]
                fld[dst, i, x, 0:8, :] = low - jnp.where(row8 == 0, low_y, 0.0)
                high = fld[dst, i, x, 8:16, :] - part[8:16]
                fld[dst, i, x, 8:16, :] = high - jnp.where(row8 == 7, high_y, 0.0)

        pl.when(r < n_res - 1)(x_up.wait_send)
        pl.when(r > 0)(x_dn.wait_send)
        pl.when(g < n_grp - 1)(y_up.wait_send)
        pl.when(g > 0)(y_dn.wait_send)
        for d in (1, 2, 3):
            c_copies[d].wait_send()
            v_copies[d].wait_send()

        for d in (1, 3, 2):
            remote(vsend.at[d], vrecv.at[par, d], v_ss.at[d], v_rs.at[par, d], (r, g)).wait_recv()

        back = [vrecv[par, d] for d in range(4)]
        for b in range(8):
            part = jnp.zeros((4, 256), F32)
            for d in range(4):
                part = jnp.where(iota4 == target[b] - 4 * d, back[d], part)
            value = jnp.sum(part, axis=0, keepdims=True)
            for i in range(3):
                term = jnp.broadcast_to(w2c[i, b : b + 1, :] * value, (32, 256))
                top = term.astype(BF16)
                rest = (term - top.astype(F32)).astype(BF16)
                for zh in range(2):
                    at = zh * 96 + i * 32
                    xs[at : at + 32, b * 256 : (b + 1) * 256] = hot[b, zh] * top
                    xs[192 + at : 192 + at + 32, b * 256 : (b + 1) * 256] = hot[b, zh] * rest
        got = jnp.dot(xs[...], spread[...], preferred_element_type=F32)
        got = got[:192] + got[192:]

        for zh in range(2):
            for i in range(3):
                for x in range(2):
                    at = zh * 96 + i * 32 + x * 16
                    zs = slice(zh * 256, (zh + 1) * 256)
                    fld[dst, i, x, :, zs] = fld[dst, i, x, :, zs] - got[at : at + 16]

        if odd:
            sums_wait(par)
        else:
            pl.when(it > 0)(lambda: sums_wait(par))
        d0, d1, d2, d3 = sums_of(par)
        rho, alpha, omega = kept(RHO), kept(ALPHA), kept(OMEGA)
        if odd:
            beta = jnp.where(first, 0.0, d0 / rho * (alpha / omega))
            alpha_next = d0 / (d1 + beta * (d2 - omega * d3))
            keep(RHO, d0)
            keep(ALPHA, alpha_next)
            keep(BETA, beta)
            outer, inner = wide(beta), wide(omega)
        else:
            omega_next = jnp.where(first, 0.0, d0 / d1)
            keep(OMEGA, omega_next)
            outer, inner = wide(-omega_next), wide(alpha)

        if odd:
            for i, x in tiles:
                old = fld[Z, i, x]
                fld[Q, i, x] = old
                fld[Z, i, x] = fld[T, i, x] + outer * (old - inner * fld[V, i, x])
        else:

            @pl.when(it > 0)
            def _():
                for i, x in tiles:
                    fld[W, i, x] = fld[Y, i, x] + outer * (fld[T, i, x] - inner * fld[V, i, x])

    def step(it, carry):
        phase(it, False)
        phase(it, True)
        return carry

    lax.fori_loop(0, ITERS, step, 0)
    sums_start(odd_rest(), 0)
    sums_on(0)
    sums_wait(0)
    inner, square, _, _ = sums_of(0)
    om, al = wide(inner / square), wide(kept(ALPHA))
    for i, x in tiles:
        q = fld[Q, i, x]
        x_out[i, x] = fld[X, i, x] + al * fld[PP, i, x] + om * q
        r_out[i, x] = q - om * fld[Y, i, x]


def hand_out(x_in, r_in, x_out, r_out, sem):
    outs = [pltpu.make_async_copy(x_in, x_out, sem.at[0]), pltpu.make_async_copy(r_in, r_out, sem.at[1])]
    for copy in outs:
        copy.start()
    for copy in outs:
        copy.wait()


def solution(mesh):
    n_res, n_grp = mesh.shape["res"], mesh.shape["grp"]
    n_dev = n_res * n_grp

    def body(right_side, accumulation, transmissibility, completion, live_count, owner, c2w, w2c, inverse):
        dma = pltpu.SemaphoreType.DMA
        field = (3, 2, 16, 512)
        any_space = pl.BlockSpec(memory_space=pl.ANY)
        vmem = pl.BlockSpec(memory_space=pltpu.VMEM)
        operands = (
            live_count,
            owner.T,
            right_side,
            accumulation,
            transmissibility,
            completion,
            jnp.transpose(c2w, (1, 0, 2)),
            jnp.transpose(w2c, (1, 0, 2)),
            inverse,
        )
        operands = [pltpu.with_memory_space_constraint(a, pltpu.HBM) for a in operands]
        held = pl.pallas_call(
            functools.partial(kernel, n_res, n_grp),
            name="bicgstab",
            out_shape=[jax.ShapeDtypeStruct(field, F32)] * 2,
            in_specs=[any_space] * 9,
            out_specs=[vmem] * 2,
            scratch_shapes=[
                pltpu.SMEM((8,), jnp.int32),
                pltpu.SMEM((1, 8), jnp.int32),
                pltpu.VMEM((11,) + field, F32),
                pltpu.VMEM((3, 3, 2, 16, 512), F32),
                pltpu.VMEM((6, 3, 3, 2, 16, 512), F32),
                pltpu.VMEM((4, 4, 256, 256), F32),
                pltpu.VMEM((8, 256), jnp.int32),
                pltpu.VMEM((3, 8, 256), F32),
                pltpu.VMEM((3, 8, 256), F32),
                pltpu.VMEM((8, 256, 256), BF16),
                pltpu.VMEM((2048, 256), BF16),
                pltpu.VMEM((8, 2, 32, 256), BF16),
                pltpu.VMEM((8, 192, 256), F32),
                pltpu.VMEM((384, 256), BF16),
                pltpu.VMEM((384, 2048), BF16),
                pltpu.VMEM((2, 2, 3, 16, 512), F32),
                pltpu.VMEM((2, 2, 8, 512), F32),
                pltpu.VMEM((2, 8, 512), F32),
                pltpu.VMEM((4, 4, 256), F32),
                pltpu.VMEM((2, 4, 4, 256), F32),
                pltpu.VMEM((4, 4, 256), F32),
                pltpu.VMEM((2, 4, 4, 256), F32),
                pltpu.VMEM((2, 2, 1, 1, 128), F32),
                pltpu.VMEM((1, 1, 128), F32),
                pltpu.VMEM((2, n_dev // 2, 1, 128), F32),
                pltpu.VMEM((4, 8, 128), F32),
                dma((18,)),
                dma((2,)),
                dma((2, 2)),
                dma((2,)),
                dma((2, 2)),
                dma((4,)),
                dma((2, 4)),
                dma((4,)),
                dma((2, 4)),
                dma(()),
                dma((2,)),
                dma(()),
                dma((2,)),
            ],
            compiler_params=pltpu.CompilerParams(
                collective_id=0, has_side_effects=True, vmem_limit_bytes=24 << 20
            ),
        )(*operands)
        return pl.pallas_call(
            hand_out,
            name="hand_out",
            out_shape=[jax.ShapeDtypeStruct(field, F32)] * 2,
            in_specs=[vmem] * 2,
            out_specs=[any_space] * 2,
            scratch_shapes=[dma((2,))],
            compiler_params=pltpu.CompilerParams(vmem_limit_bytes=1 << 20),
        )(*held)

    in_specs = (
        P(None, "res", "grp", None),
        P(None, None, "res", "grp", None),
        P(None, None, None, "res", "grp", None),
        P(RES_GRP, None),
        P(RES_GRP),
        P(RES_GRP, None),
        P(RES_GRP, None, None),
        P(RES_GRP, None, None),
        P(RES_GRP, None, None, None, None),
    )
    out_specs = (P(None, "res", "grp", None), P(None, "res", "grp", None))

    def run(*args):
        first, second = jax.shard_map(
            body, mesh=mesh, in_specs=in_specs, out_specs=out_specs, check_vma=False
        )(*args)
        return first, second

    return run
```
